8 devices in a mesh: dp: 2 (over z, y), tp: 4 (over x, core).
Axes of the slice: x: 2, y: 2, z: 1, core: 2. Of those that a mesh axis runs over, the one named last changes fastest.
Arguments:
- hidden: bfloat16 [6, 64, 4096], P('dp', 'tp'), parts along dimension 0
- ln1_gain: float32 [4096], replicated
- ln1_bias: float32 [4096], replicated
- w_qkv: bfloat16 [4096, 3, 32, 128], P(None, None, 'tp')
- b_qkv: bfloat16 [3, 32, 128], P(None, 'tp')
- w_out: bfloat16 [32, 128, 4096], P('tp')
- b_out: bfloat16 [4096], replicated
- ln2_gain: float32 [4096], replicated
- ln2_bias: float32 [4096], replicated
- w_up: bfloat16 [4096, 16384], P(None, 'tp')
- b_up: bfloat16 [16384], P('tp')
- w_down: bfloat16 [16384, 4096], P('tp')
- b_down: bfloat16 [4096], replicated
Outputs:
- output: bfloat16 [6, 64, 4096], P('dp', 'tp'), parts along dimension 0
There are 2 independent parts. The reference program is written for one: setup_inputs(seed, part) draws one part's arguments, and reference() takes and returns one part's arrays. A program takes and returns all parts, laid end to end along the dimension named above; an argument that names none is the same for every part.
All inputs are finite; a program needn't handle non-finite values.
Results may differ from the reference program's by a relative error of at most 0.010159.
Values are sent between devices in bfloat16 or wider.
A program may use at most 1 GiB of HBM per device.

```python
import math
import jax
import jax.numpy as jnp
from jax import lax

N_BATCH = 3
SEQ_LEN = 64
D_MODEL = 4096
N_HEADS = 32

HEAD_DIM = D_MODEL // N_HEADS
FF_DIM = 4 * D_MODEL
LN_EPS = 1e-5


def layer_norm(inputs, gain_vec, shift_vec):
    as_f32 = inputs.astype(jnp.float32)
    row_mean = jnp.mean(as_f32, axis=-1, keepdims=True)
    centered = as_f32 - row_mean
    variance = jnp.mean(centered * centered, axis=-1, keepdims=True)
    return (centered * lax.rsqrt(variance + LN_EPS) * gain_vec + shift_vec).astype(jnp.bfloat16)


def setup_inputs(seed: int = 0, part: int = 0) -> dict:
    root_key = jax.random.key(seed)
    sub_keys = jax.random.split(root_key, 13)
    qk_gain = (0.5 * math.log(SEQ_LEN)) ** 0.25
    col_gain = jnp.array([qk_gain, qk_gain, 1.0], jnp.float32).reshape(1, 3, 1, 1)
    hidden = jax.random.normal(jax.random.fold_in(sub_keys[0], part), (N_BATCH, SEQ_LEN, D_MODEL), jnp.float32)
    w_qkv = jax.random.normal(sub_keys[3], (D_MODEL, 3, N_HEADS, HEAD_DIM), jnp.float32) * col_gain * D_MODEL ** -0.5
    return {
        "hidden": hidden.astype(jnp.bfloat16),
        "ln1_gain": 1.0 + 0.3 * jax.random.normal(sub_keys[1], (D_MODEL,), jnp.float32),
        "ln1_bias": 0.3 * jax.random.normal(sub_keys[2], (D_MODEL,), jnp.float32),
        "w_qkv": w_qkv.astype(jnp.bfloat16),
        "b_qkv": (0.5 * jax.random.normal(sub_keys[4], (3, N_HEADS, HEAD_DIM), jnp.float32)).astype(jnp.bfloat16),
        "w_out": (jax.random.normal(sub_keys[5], (N_HEADS, HEAD_DIM, D_MODEL), jnp.float32) * D_MODEL ** -0.5).astype(jnp.bfloat16),
        "b_out": (0.3 * jax.random.normal(sub_keys[6], (D_MODEL,), jnp.float32)).astype(jnp.bfloat16),
        "ln2_gain": 1.0 + 0.3 * jax.random.normal(sub_keys[7], (D_MODEL,), jnp.float32),
        "ln2_bias": 0.3 * jax.random.normal(sub_keys[8], (D_MODEL,), jnp.float32),
        "w_up": (jax.random.normal(sub_keys[9], (D_MODEL, FF_DIM), jnp.float32) * D_MODEL ** -0.5).astype(jnp.bfloat16),
        "b_up": (0.5 * jax.random.normal(sub_keys[10], (FF_DIM,), jnp.float32)).astype(jnp.bfloat16),
        "w_down": (jax.random.normal(sub_keys[11], (FF_DIM, D_MODEL), jnp.float32) * FF_DIM ** -0.5).astype(jnp.bfloat16),
        "b_down": (0.3 * jax.random.normal(sub_keys[12], (D_MODEL,), jnp.float32)).astype(jnp.bfloat16),
    }


def reference(hidden, ln1_gain, ln1_bias, w_qkv, b_qkv, w_out, b_out, ln2_gain, ln2_bias, w_up, b_up, w_down, b_down):
    normed = layer_norm(hidden, ln1_gain, ln1_bias).reshape(N_BATCH * SEQ_LEN, D_MODEL)
    qkv_acc = jnp.dot(normed, w_qkv.reshape(D_MODEL, 3 * D_MODEL), preferred_element_type=jnp.float32)
    qkv_all = (qkv_acc + b_qkv.reshape(3 * D_MODEL).astype(jnp.float32)).astype(jnp.bfloat16)
    head_major = jnp.transpose(qkv_all.reshape(N_BATCH, SEQ_LEN, 3, N_HEADS, HEAD_DIM), (2, 3, 0, 1, 4))
    positions = jnp.arange(SEQ_LEN)
    causal = positions[:, None] >= positions[None, :]

    def one_head(operands):
        queries, keys_all, values = operands
        logits = jnp.einsum("bqd,bkd->bqk", queries.astype(jnp.float32), keys_all.astype(jnp.float32)) * HEAD_DIM ** -0.5
        logits = jnp.where(causal, logits, -1e30)
        row_max = jnp.max(logits, axis=-1, keepdims=True)
        exp_vals = jnp.exp(logits - row_max)
        weights_bf = (exp_vals / jnp.sum(exp_vals, axis=-1, keepdims=True)).astype(jnp.bfloat16)
        return jnp.einsum("bqk,bkd->bqd", weights_bf.astype(jnp.float32), values.astype(jnp.float32)).astype(jnp.bfloat16)

    context = lax.map(one_head, (head_major[0], head_major[1], head_major[2]))
    attn_sum = jnp.einsum("hbsd,hde->bse", context.astype(jnp.float32), w_out.astype(jnp.float32))
    resid_mid = (hidden.astype(jnp.float32) + (attn_sum + b_out.astype(jnp.float32))).astype(jnp.bfloat16)
    normed_mid = layer_norm(resid_mid, ln2_gain, ln2_bias).reshape(N_BATCH * SEQ_LEN, D_MODEL)
    up_proj = jnp.dot(normed_mid, w_up, preferred_element_type=jnp.float32) + b_up.astype(jnp.float32)
    gelu_out = jax.nn.gelu(up_proj, approximate=True).astype(jnp.bfloat16)
    down_sum = jnp.dot(gelu_out, w_down, preferred_element_type=jnp.float32) + b_down.astype(jnp.float32)
    return (resid_mid.astype(jnp.float32) + down_sum.reshape(N_BATCH, SEQ_LEN, D_MODEL)).astype(jnp.bfloat16)
```

```python
import jax
import jax.numpy as jnp
from jax import lax
from jax.experimental import pallas as pl
from jax.experimental.pallas import tpu as pltpu
from jax.sharding import PartitionSpec as P

MESH = pl.DeviceIdType.MESH
F32, BF16 = jnp.float32, jnp.bfloat16

LN_EPS = 1e-5
N_BATCH, BLOCK, D = 3, 16, 4096
ROWS = N_BATCH * BLOCK
TOKENS = 4 * ROWS
HEADS, HEAD_DIM = 8, 128
FF = 4096
QKV = 3 * HEADS * HEAD_DIM

PK, PN = 1024, 512
KC = D // PK
NC = D // PN
N_QKV, N_OUT, N_UP, N_DOWN = 24, 8, 32, 32
G_OUT, G_UP, G_DOWN = 24, 32, 64
SLOTS = 36
STAGE_ROWS, STAGES = 256, 4
STEPS = D // STAGE_ROWS


def kernel(x_hbm, g1_hbm, b1_hbm, wqkv_hbm, bqkv_hbm, wout_hbm, bout_hbm, g2_hbm, b2_hbm, wup_hbm, bup_hbm, wdown_hbm, bdown_hbm, out_hbm,
           stage, slots, x_own, h_all, x1_all, acc, qkv_bf, ctx, u, own, pf,
           psend1, prec1, xsend1, xrec1, psend2, prec2, xsend2, xrec2, xsum, stats, ostage,
           vec_f32, vec_bf, bqkv_v, rows, bqkv_row,
           stage_sem, slot_sem, small_sem, x_sem, out_sem,
           ag_s, ag_r, ag2_s, ag2_r, st_s, st_r, rs1_s, rs1_r, rs2_s, rs2_r):
    dp = lax.axis_index("dp")
    me = lax.axis_index("tp")
    core = lax.rem(me, 2)
    chip = lax.div(me, 2)
    partner = me + 1 - 2 * core
    cross = lax.rem(me + 2, 4)
    far = lax.rem(partner + 2, 4)
    other_core = 1 - core
    other_chip = 1 - chip

    def stage_copy(i):
        return pltpu.make_async_copy(wqkv_hbm.at[pl.ds(i * STAGE_ROWS, STAGE_ROWS)], stage.at[lax.rem(i, STAGES)], stage_sem.at[lax.rem(i, STAGES)])

    def to_slot(src, g):
        s = lax.rem(g, SLOTS)
        return pltpu.make_async_copy(src, slots.at[s], slot_sem.at[s])

    def out_copy(n):
        return to_slot(wout_hbm.at[:, pl.ds(n * PN, PN)], G_OUT + n)

    def up_copy(i):
        k, n = lax.div(i, NC), lax.rem(i, NC)
        return to_slot(wup_hbm.at[pl.ds(pl.multiple_of(k * PK, PK), PK), pl.ds(pl.multiple_of(n * PN, PN), PN)], G_UP + i)

    def down_copy(i):
        n, k = lax.div(i, KC), lax.rem(i, KC)
        return to_slot(wdown_hbm.at[pl.ds(pl.multiple_of(k * PK, PK), PK), pl.ds(pl.multiple_of(n * PN, PN), PN)], G_DOWN + i)

    x_copy = pltpu.make_async_copy(x_hbm, x_own, x_sem.at[0])
    x_copy.start()
    smalls = [pltpu.make_async_copy(src, vec_f32.at[i], small_sem.at[i]) for i, src in enumerate((g1_hbm, b1_hbm, g2_hbm, b2_hbm))]
    smalls += [pltpu.make_async_copy(src, vec_bf.at[i], small_sem.at[4 + i]) for i, src in enumerate((bout_hbm, bup_hbm, bdown_hbm))]
    smalls += [pltpu.make_async_copy(bqkv_hbm, bqkv_v, small_sem.at[7])]
    for c in smalls:
        c.start()
    for i in range(STAGES):
        stage_copy(i).start()

    barrier = pltpu.get_barrier_semaphore()
    for peer in (partner, cross):
        pl.semaphore_signal(barrier, inc=1, device_id=(dp, peer), device_id_type=MESH)

    for c in smalls:
        c.wait()
    for i in range(4):
        for j in range(32):
            rows[i, :, j * 128:(j + 1) * 128] = vec_f32[i, j:j + 1, :]
    for i in range(3):
        vals = vec_bf[i].astype(F32)
        for j in range(32):
            rows[4 + i, :, j * 128:(j + 1) * 128] = vals[j:j + 1, :]
    for t in range(3):
        vals = bqkv_v[t].astype(F32)
        for j in range(HEADS):
            bqkv_row[:, (t * HEADS + j) * 128:(t * HEADS + j + 1) * 128] = vals[j:j + 1, :]
    G1, B1, G2, B2, BOUT, BUP, BDOWN = range(7)

    def row_stats(x):
        mean = jnp.mean(x, axis=-1, keepdims=True)
        centered = x - mean
        var = jnp.mean(centered * centered, axis=-1, keepdims=True)
        return mean, lax.rsqrt(var + LN_EPS)

    x_copy.wait()
    for b in range(N_BATCH):
        r = pl.ds(b * BLOCK, BLOCK)
        xf = x_own[r, :].astype(F32)
        mean, rstd = row_stats(xf)
        h_all[me, r, :] = ((xf - mean) * rstd * rows[G1] + rows[B1]).astype(BF16)

    pl.semaphore_wait(barrier, 2)

    def push(buf, block, c, width, s, r, which, peer):
        ref = buf.at[block, :, pl.ds(c * width, width)]
        return pltpu.make_async_remote_copy(src_ref=ref, dst_ref=ref, send_sem=s.at[which, c], recv_sem=r.at[which, c], device_id=(dp, peer), device_id_type=MESH)

    def ag1(which, block, peer, c):
        return push(h_all, block, c, PK, ag_s, ag_r, which, peer)

    for c in range(KC):
        ag1(0, me, cross, c).start()
    for c in range(KC):
        ag1(1, me, partner, c).start()

    def ag1_forward(c):
        ag1(0, cross, cross, c).wait_recv()
        ag1(2, cross, partner, c).start()

    def relayout(i, carry):
        stage_copy(i).wait()
        s = lax.rem(i, STAGES)
        k, off = lax.div(i, 4), lax.rem(i, 4)
        r = pl.ds(pl.multiple_of(off * STAGE_ROWS, STAGE_ROWS), STAGE_ROWS)
        for t in range(3):
            w = stage[s, :, t].reshape(STAGE_ROWS, HEADS * HEAD_DIM)
            slots[k * 6 + 2 * t, r, :] = w[:, :PN]
            slots[k * 6 + 2 * t + 1, r, :] = w[:, PN:]

        @pl.when(i + STAGES < STEPS)
        def _():
            stage_copy(i + STAGES).start()

        return carry

    lax.fori_loop(0, STEPS - STAGES, relayout, 0)
    for n in range(N_OUT):
        out_copy(n).start()
    for i in range(SLOTS - G_UP):
        up_copy(i).start()
    lax.fori_loop(STEPS - STAGES, STEPS, relayout, 0)

    def tokens(buf, c):
        return buf[:, :, c * PK:(c + 1) * PK].reshape(TOKENS, PK)

    def qkv_chunk(c):
        ag1(1, partner, partner, c).wait_recv()
        ag1(2, far, partner, c).wait_recv()
        h = tokens(h_all, c)

        def group(q, carry):
            for m in range(3):
                n = q * 3 + m
                cols = pl.ds(pl.multiple_of(n * PN, PN), PN)
                part = jnp.dot(h, slots[c * 6 + n], preferred_element_type=F32)
                if c:
                    part = part + acc[:, cols]
                if c < KC - 1:
                    acc[:, cols] = part
                else:
                    val = (part + bqkv_row[:, cols]).astype(BF16)
                    for d in range(4):
                        for b in range(N_BATCH):
                            qkv_bf[b, d * BLOCK:(d + 1) * BLOCK, cols] = val[d * ROWS + b * BLOCK:d * ROWS + (b + 1) * BLOCK]
            for m in range(3):
                up_copy(c * 6 + q * 3 + m + SLOTS - G_UP).start()
            return carry

        lax.fori_loop(0, 2, group, 0)

    ag1_forward(0)
    ag1_forward(1)
    qkv_chunk(0)
    ag1_forward(2)
    qkv_chunk(1)
    ag1_forward(3)
    qkv_chunk(2)
    qkv_chunk(3)
    for c in range(KC):
        ag1(0, me, cross, c).wait_send()
        ag1(1, me, partner, c).wait_send()
        ag1(2, cross, partner, c).wait_send()

    def attend(b, carry):
        seq = N_BATCH * 0 + 4 * BLOCK
        causal = lax.broadcasted_iota(jnp.int32, (seq, seq), 0) >= lax.broadcasted_iota(jnp.int32, (seq, seq), 1)
        r = pl.ds(pl.multiple_of(b * BLOCK, BLOCK), BLOCK)
        for j in range(HEADS):
            q, k, v = (qkv_bf[b, :, (t * HEADS + j) * HEAD_DIM:(t * HEADS + j + 1) * HEAD_DIM] for t in range(3))
            logits = lax.dot_general(q, k, (((1,), (1,)), ((), ())), preferred_element_type=F32) * HEAD_DIM ** -0.5
            logits = jnp.where(causal, logits, -1e30)
            e = jnp.exp(logits - jnp.max(logits, axis=-1, keepdims=True))
            p = (e * (1.0 / jnp.sum(e, axis=-1, keepdims=True))).astype(BF16)
            o = jnp.dot(p, v, preferred_element_type=F32).astype(BF16)
            for d in range(4):
                ctx[d, r, j * HEAD_DIM:(j + 1) * HEAD_DIM] = o[d * BLOCK:(d + 1) * BLOCK]
        return carry

    lax.fori_loop(0, N_BATCH, attend, 0)

    def rs_pair(psend, prec, s, r, n):
        return pltpu.make_async_remote_copy(src_ref=psend.at[n], dst_ref=prec.at[n], send_sem=s.at[0, n], recv_sem=r.at[0, n], device_id=(dp, partner), device_id_type=MESH)

    def rs_cross(xsend, xrec, s, r, n):
        return pltpu.make_async_remote_copy(src_ref=xsend.at[n], dst_ref=xrec.at[n], send_sem=s.at[1, n], recv_sem=r.at[1, n], device_id=(dp, cross), device_id_type=MESH)

    def rs_a(part, psend, prec, s, r, n):
        pf[...] = part.reshape(4, ROWS, PN)
        for q in range(2):
            psend[n, q] = pf[2 * q + other_core].astype(BF16)
            own[n, q] = pf[2 * q + core]
        rs_pair(psend, prec, s, r, n).start()

    def rs_b(psend, prec, xsend, xrec, s, r, n):
        rs_pair(psend, prec, s, r, n).wait_recv()
        xsend[n] = (own[n, other_chip] + prec[n, other_chip].astype(F32)).astype(BF16)
        rs_cross(xsend, xrec, s, r, n).start()
        xsum[n] = own[n, chip] + prec[n, chip].astype(F32)

    def rs_c(xsend, xrec, s, r, n):
        rs_cross(xsend, xrec, s, r, n).wait_recv()
        return xsum[n] + xrec[n].astype(F32)

    ctx_rows = ctx[...].reshape(TOKENS, HEADS * HEAD_DIM)

    def out_a(n):
        out_copy(n).wait()
        rs_a(jnp.dot(ctx_rows, slots[(G_OUT + n) % SLOTS], preferred_element_type=F32), psend1, prec1, rs1_s, rs1_r, n)
        g = G_OUT + n + SLOTS
        (up_copy(g - G_UP) if g < G_DOWN else down_copy(g - G_DOWN)).start()

    def out_b(n):
        rs_b(psend1, prec1, xsend1, xrec1, rs1_s, rs1_r, n)

    def ag2(which, block, peer, c):
        return push(x1_all, block, c, PK, ag2_s, ag2_r, which, peer)

    def st(which, block, peer):
        ref = stats.at[block]
        return pltpu.make_async_remote_copy(src_ref=ref, dst_ref=ref, send_sem=st_s.at[which], recv_sem=st_r.at[which], device_id=(dp, peer), device_id_type=MESH)

    lead = 4
    for n in range(NC):
        out_a(n)
        if n >= lead:
            out_b(n - lead)
    for n in range(NC - lead, NC):
        out_b(n)
    for n in range(NC):
        cols = slice(n * PN, (n + 1) * PN)
        total = rs_c(xsend1, xrec1, rs1_s, rs1_r, n)
        x1_all[me, :, cols] = (x_own[:, cols].astype(F32) + (total + rows[BOUT, :, cols])).astype(BF16)
        if n == 1:
            ag2(0, me, cross, 0).start()
            ag2(1, me, partner, 0).start()
    for b in range(N_BATCH):
        r = pl.ds(b * BLOCK, BLOCK)
        mean, rstd = row_stats(x1_all[me, r, :].astype(F32))
        lane = lax.broadcasted_iota(jnp.int32, (BLOCK, 128), 1)
        stats[me, r, :] = jnp.where(lane == 0, mean, rstd)
    st(0, me, cross).start()
    st(1, me, partner).start()
    for c in range(1, KC):
        ag2(0, me, cross, c).start()
        ag2(1, me, partner, c).start()
    st(0, cross, cross).wait_recv()
    st(2, cross, partner).start()

    def ag2_forward(c):
        ag2(0, cross, cross, c).wait_recv()
        ag2(2, cross, partner, c).start()

    def up_chunk(c):
        ag2(1, partner, partner, c).wait_recv()
        ag2(2, far, partner, c).wait_recv()
        cols = slice(c * PK, (c + 1) * PK)
        for d in range(4):
            xf = x1_all[d, :, cols].astype(F32)
            h_all[d, :, cols] = ((xf - stats[d, :, 0:1]) * stats[d, :, 1:2] * rows[G2, :, cols] + rows[B2, :, cols]).astype(BF16)
        h = tokens(h_all, c)

        def group(q, carry):
            for m in range(4):
                up_copy(c * NC + q * 4 + m).wait()
            for m in range(4):
                n = q * 4 + m
                wide = pl.ds(pl.multiple_of(n * PN, PN), PN)
                part = jnp.dot(h, slots[lax.rem(G_UP + c * NC + n, SLOTS)], preferred_element_type=F32)
                if c:
                    part = part + acc[:, wide]
                if c < KC - 1:
                    acc[:, wide] = part
                else:
                    u[:, wide] = jax.nn.gelu(part + rows[BUP, :, wide], approximate=True).astype(BF16)
            for m in range(4):
                i = c * NC + q * 4 + m + G_UP + SLOTS - G_DOWN

                @pl.when(i < N_DOWN)
                def _():
                    down_copy(i).start()

            return carry

        lax.fori_loop(0, 2, group, 0)

    ag2_forward(0)
    st(1, partner, partner).wait_recv()
    st(2, far, partner).wait_recv()
    ag2_forward(1)
    up_chunk(0)
    ag2_forward(2)
    up_chunk(1)
    ag2_forward(3)
    up_chunk(2)
    up_chunk(3)

    def down_a(n):
        for k in range(KC):
            down_copy(n * KC + k).wait()
        part = None
        for k in range(KC):
            term = jnp.dot(u[:, k * PK:(k + 1) * PK], slots[(G_DOWN + n * KC + k) % SLOTS], preferred_element_type=F32)
            part = term if part is None else part + term
        rs_a(part, psend2, prec2, rs2_s, rs2_r, n)

    def out_write(n):
        cols = pl.ds(n * PN, PN)
        return pltpu.make_async_copy(ostage.at[:, cols], out_hbm.at[:, cols], out_sem.at[n])

    def down_b(n):
        rs_b(psend2, prec2, xsend2, xrec2, rs2_s, rs2_r, n)

    def down_c(n):
        cols = slice(n * PN, (n + 1) * PN)
        total = rs_c(xsend2, xrec2, rs2_s, rs2_r, n)
        ostage[:, cols] = (x1_all[me, :, cols].astype(F32) + (total + rows[BDOWN, :, cols])).astype(BF16)
        out_write(n).start()

    for n in range(NC):
        down_a(n)
        if n >= 1:
            down_b(n - 1)
    down_b(NC - 1)
    for n in range(NC):
        down_c(n)

    for n in range(NC):
        out_write(n).wait()
        rs_pair(psend1, prec1, rs1_s, rs1_r, n).wait_send()
        rs_cross(xsend1, xrec1, rs1_s, rs1_r, n).wait_send()
        rs_pair(psend2, prec2, rs2_s, rs2_r, n).wait_send()
        rs_cross(xsend2, xrec2, rs2_s, rs2_r, n).wait_send()
    for c in range(KC):
        ag2(0, me, cross, c).wait_send()
        ag2(1, me, partner, c).wait_send()
        ag2(2, cross, partner, c).wait_send()
    st(0, me, cross).wait_send()
    st(1, me, partner).wait_send()
    st(2, cross, partner).wait_send()


def solution(mesh):
    def device_body(hidden, ln1_gain, ln1_bias, w_qkv, b_qkv, w_out, b_out, ln2_gain, ln2_bias, w_up, b_up, w_down, b_down):
        args = (hidden.reshape(ROWS, D), ln1_gain.reshape(32, 128), ln1_bias.reshape(32, 128), w_qkv, b_qkv, w_out.reshape(HEADS * HEAD_DIM, D),
                b_out.reshape(32, 128), ln2_gain.reshape(32, 128), ln2_bias.reshape(32, 128), w_up, b_up.reshape(32, 128), w_down, b_down.reshape(32, 128))
        hbm = pl.BlockSpec(memory_space=pltpu.HBM)
        dma = pltpu.SemaphoreType.DMA
        rs_buffers = [pltpu.VMEM((NC, 2, ROWS, PN), BF16), pltpu.VMEM((NC, 2, ROWS, PN), BF16), pltpu.VMEM((NC, ROWS, PN), BF16), pltpu.VMEM((NC, ROWS, PN), BF16)]
        result = pl.pallas_call(
            kernel,
            out_shape=jax.ShapeDtypeStruct((ROWS, D), BF16),
            in_specs=[hbm] * len(args),
            out_specs=hbm,
            scratch_shapes=[
                pltpu.VMEM((STAGES, STAGE_ROWS, 3, HEADS, HEAD_DIM), BF16),
                pltpu.VMEM((SLOTS, PK, PN), BF16),
                pltpu.VMEM((ROWS, D), BF16),
                pltpu.VMEM((4, ROWS, D), BF16),
                pltpu.VMEM((4, ROWS, D), BF16),
                pltpu.VMEM((TOKENS, FF), F32),
                pltpu.VMEM((N_BATCH, 4 * BLOCK, QKV), BF16),
                pltpu.VMEM((4, ROWS, HEADS * HEAD_DIM), BF16),
                pltpu.VMEM((TOKENS, FF), BF16),
                pltpu.VMEM((NC, 2, ROWS, PN), F32),
                pltpu.VMEM((4, ROWS, PN), F32),
                *rs_buffers,
                *rs_buffers,
                pltpu.VMEM((NC, ROWS, PN), F32),
                pltpu.VMEM((4, ROWS, 128), F32),
                pltpu.VMEM((ROWS, D), BF16),
                pltpu.VMEM((4, 32, 128), F32),
                pltpu.VMEM((3, 32, 128), BF16),
                pltpu.VMEM((3, HEADS, HEAD_DIM), BF16),
                pltpu.VMEM((7, 1, D), F32),
                pltpu.VMEM((1, QKV), F32),
                dma((STAGES,)), dma((SLOTS,)), dma((8,)), dma((1,)), dma((NC,)),
                dma((3, KC)), dma((3, KC)), dma((3, KC)), dma((3, KC)), dma((3,)), dma((3,)),
                dma((2, NC)), dma((2, NC)), dma((2, NC)), dma((2, NC)),
            ],
            compiler_params=pltpu.CompilerParams(collective_id=0, has_side_effects=True, vmem_limit_bytes=67_043_328),
            name="decoder_layer",
        )(*args)
        return result.reshape(hidden.shape)

    in_layout = (P("dp", "tp", None), P(), P(), P(None, None, "tp", None), P(None, "tp", None), P("tp", None, None), P(), P(), P(), P(None, "tp"), P("tp"), P("tp", None), P())
    return jax.shard_map(device_body, mesh=mesh, in_specs=in_layout, out_specs=P("dp", "tp", None), check_vma=False)
```

```python
import jax
import jax.numpy as jnp
from jax import lax
from jax.experimental import pallas as pl
from jax.experimental.pallas import tpu as pltpu
from jax.sharding import PartitionSpec as P

MESH = pl.DeviceIdType.MESH
F32, BF16 = jnp.float32, jnp.bfloat16

LN_EPS = 1e-5
N_BATCH, BLOCK, D = 3, 16, 4096
ROWS = N_BATCH * BLOCK
TOKENS = 4 * ROWS
HEADS, HEAD_DIM = 8, 128
FF = 4096
QKV = 3 * HEADS * HEAD_DIM

PK, PN = 1024, 512
KC = D // PK
NC = D // PN
N_QKV, N_OUT, N_UP, N_DOWN = 24, 8, 32, 32
G_OUT, G_UP, G_DOWN = 24, 32, 64
SLOTS = 36
STAGE_ROWS, STAGES = 256, 4
STEPS = D // STAGE_ROWS


def kernel(x_hbm, g1_hbm, b1_hbm, wqkv_hbm, bqkv_hbm, wout_hbm, bout_hbm, g2_hbm, b2_hbm, wup_hbm, bup_hbm, wdown_hbm, bdown_hbm, out_ref,
           stage, slots, x_own, h_all, x1_all, acc, qkv_bf, ctx, u, own, pf,
           psend1, prec1, xsend1, xrec1, psend2, prec2, xsend2, xrec2, xsum, stats, stat_cols, square,
           vec_f32, vec_bf, bqkv_v, rows, bqkv_row, mask,
           stage_sem, slot_sem, small_sem, x_sem,
           ag_s, ag_r, ag2_s, ag2_r, st_s, st_r, rs1_s, rs1_r, rs2_s, rs2_r):
    dp = lax.axis_index("dp")
    me = lax.axis_index("tp")
    core = lax.rem(me, 2)
    chip = lax.div(me, 2)
    partner = me + 1 - 2 * core
    cross = lax.rem(me + 2, 4)
    far = lax.rem(partner + 2, 4)
    other_core = 1 - core
    other_chip = 1 - chip

    def stage_copy(i):
        return pltpu.make_async_copy(wqkv_hbm.at[pl.ds(i * STAGE_ROWS, STAGE_ROWS)], stage.at[lax.rem(i, STAGES)], stage_sem.at[lax.rem(i, STAGES)])

    def to_slot(src, g):
        s = lax.rem(g, SLOTS)
        return pltpu.make_async_copy(src, slots.at[s], slot_sem.at[s])

    def out_copy(n):
        return to_slot(wout_hbm.at[:, pl.ds(n * PN, PN)], G_OUT + n)

    def up_copy(i):
        k, n = lax.div(i, NC), lax.rem(i, NC)
        return to_slot(wup_hbm.at[pl.ds(pl.multiple_of(k * PK, PK), PK), pl.ds(pl.multiple_of(n * PN, PN), PN)], G_UP + i)

    def down_copy(i):
        n, k = lax.div(i, KC), lax.rem(i, KC)
        return to_slot(wdown_hbm.at[pl.ds(pl.multiple_of(k * PK, PK), PK), pl.ds(pl.multiple_of(n * PN, PN), PN)], G_DOWN + i)

    barrier = pltpu.get_barrier_semaphore()
    for peer in (partner, cross, far):
        pl.semaphore_signal(barrier, inc=1, device_id=(dp, peer), device_id_type=MESH)
    G1, B1, G2, B2, BOUT, BUP, BDOWN = range(7)
    x_copy = pltpu.make_async_copy(x_hbm, x_own, x_sem.at[0])
    smalls = [pltpu.make_async_copy(src, vec_f32.at[i], small_sem.at[i]) for i, src in enumerate((g1_hbm, b1_hbm, g2_hbm, b2_hbm))]
    smalls += [pltpu.make_async_copy(src, vec_bf.at[i], small_sem.at[4 + i]) for i, src in enumerate((bout_hbm, bup_hbm, bdown_hbm))]
    smalls += [pltpu.make_async_copy(bqkv_hbm, bqkv_v, small_sem.at[7])]
    smalls[G1].start()
    smalls[B1].start()
    x_copy.start()

    def f32_row(i):
        for j in range(32):
            rows[i, :, j * 128:(j + 1) * 128] = vec_f32[i, j:j + 1, :]

    def row_stats(x):
        mean = jnp.mean(x, axis=-1, keepdims=True)
        centered = x - mean
        var = jnp.mean(centered * centered, axis=-1, keepdims=True)
        return mean, lax.rsqrt(var + LN_EPS)

    for i in (G1, B1):
        smalls[i].wait()
        f32_row(i)
    x_copy.wait()
    for i in range(STAGES):
        stage_copy(i).start()
    for c in smalls[2:]:
        c.start()
    for b in range(N_BATCH):
        r = pl.ds(b * BLOCK, BLOCK)
        xf = x_own[r, :].astype(F32)
        mean, rstd = row_stats(xf)
        h_all[me, r, :] = ((xf - mean) * rstd * rows[G1] + rows[B1]).astype(BF16)

    pl.semaphore_wait(barrier, 3)

    def push(buf, block, c, width, s, r, which, peer):
        ref = buf.at[block, :, pl.ds(c * width, width)]
        return pltpu.make_async_remote_copy(src_ref=ref, dst_ref=ref, send_sem=s.at[which, c], recv_sem=r.at[which, c], device_id=(dp, peer), device_id_type=MESH)

    def ag1(which, block, peer, c):
        return push(h_all, block, c, PK, ag_s, ag_r, which, peer)

    for c in range(KC):
        ag1(0, me, cross, c).start()
    for c in range(KC):
        ag1(1, me, partner, c).start()

    for c in smalls[2:]:
        c.wait()
    for i in (G2, B2):
        f32_row(i)
    for i in range(3):
        vals = vec_bf[i].astype(F32)
        for j in range(32):
            rows[4 + i, :, j * 128:(j + 1) * 128] = vals[j:j + 1, :]
    for t in range(3):
        vals = bqkv_v[t].astype(F32)
        for j in range(HEADS):
            bqkv_row[:, (t * HEADS + j) * 128:(t * HEADS + j + 1) * 128] = vals[j:j + 1, :]

    def token_place(axis):
        t = lax.broadcasted_iota(jnp.int32, (TOKENS, TOKENS), axis)
        d = sum((t >= ROWS * i).astype(jnp.int32) for i in range(1, 4))
        t = t - ROWS * d
        b = sum((t >= BLOCK * i).astype(jnp.int32) for i in range(1, N_BATCH))
        return b, d * BLOCK + t - BLOCK * b

    (q_seq, q_pos), (k_seq, k_pos) = token_place(0), token_place(1)
    square[...] = jnp.zeros_like(square)
    mask[...] = ((q_seq == k_seq) & (q_pos >= k_pos)).astype(F32)

    def ag1_forward(c):
        ag1(0, cross, cross, c).wait_recv()
        ag1(2, cross, partner, c).start()

    def relayout(i):
        s = lax.rem(i, STAGES)
        k, off = lax.div(i, 4), lax.rem(i, 4)
        r = pl.ds(pl.multiple_of(off * STAGE_ROWS, STAGE_ROWS), STAGE_ROWS)
        for t in range(3):
            w = stage[s, :, t].reshape(STAGE_ROWS, HEADS * HEAD_DIM)
            slots[k * 6 + 2 * t, r, :] = w[:, :PN]
            slots[k * 6 + 2 * t + 1, r, :] = w[:, PN:]

    def relayout_step(i, carry):
        stage_copy(i).wait()
        relayout(i)

        @pl.when(i + STAGES < STEPS)
        def _():
            stage_copy(i + STAGES).start()

        return carry

    lax.fori_loop(0, STEPS - STAGES, relayout_step, 0)
    for n in range(N_OUT):
        out_copy(n).start()
    for i in range(SLOTS - G_UP):
        up_copy(i).start()
    lax.fori_loop(STEPS - STAGES, STEPS, relayout_step, 0)

    def tokens(buf, c):
        return buf[:, :, c * PK:(c + 1) * PK].reshape(TOKENS, PK)

    def qkv_chunk(c):
        ag1(1, partner, partner, c).wait_recv()
        ag1(2, far, partner, c).wait_recv()
        h = tokens(h_all, c)
        for n in range(6):
            cols = slice(n * PN, (n + 1) * PN)
            part = jnp.dot(h, slots[c * 6 + n], preferred_element_type=F32)
            if c:
                part = part + acc[:, cols]
            if c < KC - 1:
                acc[:, cols] = part
            else:
                qkv_bf[:, cols] = (part + bqkv_row[:, cols]).astype(BF16)
        for n in range(6):
            up_copy(c * 6 + n + SLOTS - G_UP).start()

    ag1_forward(0)
    for c in range(KC):
        if c < KC - 1:
            ag1_forward(c + 1)
        qkv_chunk(c)
    for c in range(KC):
        ag1(0, me, cross, c).wait_send()
        ag1(1, me, partner, c).wait_send()
        ag1(2, cross, partner, c).wait_send()

    keep = mask[...] > 0.5
    for first in range(0, HEADS, 4):
        heads = range(first, first + 4)

        def part_of(t, j):
            return qkv_bf[:, (t * HEADS + j) * HEAD_DIM:(t * HEADS + j + 1) * HEAD_DIM]

        logits = [lax.dot_general(part_of(0, j), part_of(1, j), (((1,), (1,)), ((), ())), preferred_element_type=F32) for j in heads]
        logits = [jnp.where(keep, x * HEAD_DIM ** -0.5, -1e30) for x in logits]
        tops = [jnp.max(x, axis=-1, keepdims=True) for x in logits]
        es = [jnp.exp(x - t) for x, t in zip(logits, tops)]
        sums = [jnp.sum(e, axis=-1, keepdims=True) for e in es]
        ps = [(e * (1.0 / z)).astype(BF16) for e, z in zip(es, sums)]
        for j, p in zip(heads, ps):
            ctx[:, j * HEAD_DIM:(j + 1) * HEAD_DIM] = jnp.dot(p, part_of(2, j), preferred_element_type=F32).astype(BF16)

    def rs_pair(psend, prec, s, r, n):
        return pltpu.make_async_remote_copy(src_ref=psend.at[n], dst_ref=prec.at[n], send_sem=s.at[0, n], recv_sem=r.at[0, n], device_id=(dp, partner), device_id_type=MESH)

    def rs_cross(xsend, xrec, s, r, n):
        return pltpu.make_async_remote_copy(src_ref=xsend.at[n], dst_ref=xrec.at[n], send_sem=s.at[1, n], recv_sem=r.at[1, n], device_id=(dp, cross), device_id_type=MESH)

    def rs_a(part, psend, prec, s, r, n):
        pf[...] = part.reshape(4, ROWS, PN)
        for q in range(2):
            psend[n, q] = pf[2 * q + other_core].astype(BF16)
            own[n, q] = pf[2 * q + core]
        rs_pair(psend, prec, s, r, n).start()

    def rs_b(psend, prec, xsend, xrec, s, r, n):
        rs_pair(psend, prec, s, r, n).wait_recv()
        xsend[n] = (own[n, other_chip] + prec[n, other_chip].astype(F32)).astype(BF16)
        rs_cross(xsend, xrec, s, r, n).start()
        xsum[n] = own[n, chip] + prec[n, chip].astype(F32)

    def rs_c(xsend, xrec, s, r, n):
        rs_cross(xsend, xrec, s, r, n).wait_recv()
        return xsum[n] + xrec[n].astype(F32)

    ctx_rows = ctx[...]

    def out_a(n):
        out_copy(n).wait()
        rs_a(jnp.dot(ctx_rows, slots[(G_OUT + n) % SLOTS], preferred_element_type=F32), psend1, prec1, rs1_s, rs1_r, n)
        g = G_OUT + n + SLOTS
        (up_copy(g - G_UP) if g < G_DOWN else down_copy(g - G_DOWN)).start()

    def out_b(n):
        rs_b(psend1, prec1, xsend1, xrec1, rs1_s, rs1_r, n)

    def ag2(which, block, peer, c):
        return push(x1_all, block, c, PK, ag2_s, ag2_r, which, peer)

    def st(which, block, peer):
        ref = stats.at[block]
        return pltpu.make_async_remote_copy(src_ref=ref, dst_ref=ref, send_sem=st_s.at[which], recv_sem=st_r.at[which], device_id=(dp, peer), device_id_type=MESH)

    lead = 3
    for n in range(NC):
        out_a(n)
        if n >= lead:
            out_b(n - lead)
    for n in range(NC - lead, NC):
        out_b(n)
    for n in range(NC):
        cols = slice(n * PN, (n + 1) * PN)
        total = rs_c(xsend1, xrec1, rs1_s, rs1_r, n)
        x1_all[me, :, cols] = (x_own[:, cols].astype(F32) + (total + rows[BOUT, :, cols])).astype(BF16)
        if n == NC - 2:
            ag2(0, me, cross, 0).start()
            ag2(1, me, partner, 0).start()
    for b in range(N_BATCH):
        r = pl.ds(b * BLOCK, BLOCK)
        mean, rstd = row_stats(x1_all[me, r, :].astype(F32))
        lane = lax.broadcasted_iota(jnp.int32, (BLOCK, 128), 1)
        square[r, :] = jnp.where(lane == 0, mean, rstd)
    stats[me] = square[...].T[:8]
    st(0, me, cross).start()
    st(2, me, far).start()
    st(1, me, partner).start()
    for c in range(1, KC):
        ag2(0, me, cross, c).start()
        ag2(1, me, partner, c).start()

    def ag2_forward(c):
        ag2(0, cross, cross, c).wait_recv()
        ag2(2, cross, partner, c).start()

    def arrive(c):
        ag2(1, partner, partner, c).wait_recv()
        ag2(2, far, partner, c).wait_recv()

    def normalize(c):
        cols = slice(c * PK, (c + 1) * PK)
        for d in range(4):
            xf = x1_all[d, :, cols].astype(F32)
            h_all[d, :, cols] = ((xf - stat_cols[d, :, 0:1]) * stat_cols[d, :, 1:2] * rows[G2, :, cols] + rows[B2, :, cols]).astype(BF16)

    def up_panels(c, panels):
        for n in panels:
            up_copy(c * NC + n).wait()
        h = tokens(h_all, c)
        for n in panels:
            wide = slice(n * PN, (n + 1) * PN)
            part = jnp.dot(h, slots[(G_UP + c * NC + n) % SLOTS], preferred_element_type=F32)
            if c:
                part = part + acc[:, wide]
            if c < KC - 1:
                acc[:, wide] = part
            else:
                u[:, wide] = jax.nn.gelu(part + rows[BUP, :, wide], approximate=True).astype(BF16)

    def refill(c, panels):
        for n in panels:
            i = c * NC + n + G_UP + SLOTS - G_DOWN
            if i < N_DOWN:
                down_copy(i).start()

    ag2_forward(0)
    st(1, partner, partner).wait_recv()
    st(0, cross, cross).wait_recv()
    st(2, far, far).wait_recv()
    for d in range(4):
        square[0:8, :] = stats[d]
        stat_cols[d] = square[...].T[:ROWS]
    arrive(0)
    normalize(0)
    for c in range(KC):
        up_panels(c, range(0, 4))
        refill(c, range(0, 4))
        if c < KC - 1:
            ag2_forward(c + 1)
            arrive(c + 1)
        up_panels(c, range(4, 8))
        if c < KC - 1:
            normalize(c + 1)
        refill(c, range(4, 8))

    def down_a(n):
        for k in range(KC):
            down_copy(n * KC + k).wait()
        part = None
        for k in range(KC):
            term = jnp.dot(u[:, k * PK:(k + 1) * PK], slots[(G_DOWN + n * KC + k) % SLOTS], preferred_element_type=F32)
            part = term if part is None else part + term
        rs_a(part, psend2, prec2, rs2_s, rs2_r, n)

    def down_b(n):
        rs_b(psend2, prec2, xsend2, xrec2, rs2_s, rs2_r, n)

    def down_c(n):
        cols = slice(n * PN, (n + 1) * PN)
        total = rs_c(xsend2, xrec2, rs2_s, rs2_r, n)
        out_ref[:, cols] = (x1_all[me, :, cols].astype(F32) + (total + rows[BDOWN, :, cols])).astype(BF16)

    for n in range(NC):
        down_a(n)
        if n >= 1:
            down_b(n - 1)
    down_b(NC - 1)
    for n in range(NC):
        down_c(n)

    for n in range(NC):
        rs_pair(psend1, prec1, rs1_s, rs1_r, n).wait_send()
        rs_cross(xsend1, xrec1, rs1_s, rs1_r, n).wait_send()
        rs_pair(psend2, prec2, rs2_s, rs2_r, n).wait_send()
        rs_cross(xsend2, xrec2, rs2_s, rs2_r, n).wait_send()
    for c in range(KC):
        ag2(0, me, cross, c).wait_send()
        ag2(1, me, partner, c).wait_send()
        ag2(2, cross, partner, c).wait_send()
    st(0, me, cross).wait_send()
    st(1, me, partner).wait_send()
    st(2, me, far).wait_send()


def solution(mesh):
    def device_body(hidden, ln1_gain, ln1_bias, w_qkv, b_qkv, w_out, b_out, ln2_gain, ln2_bias, w_up, b_up, w_down, b_down):
        args = (hidden.reshape(ROWS, D), ln1_gain.reshape(32, 128), ln1_bias.reshape(32, 128), w_qkv, b_qkv, w_out.reshape(HEADS * HEAD_DIM, D),
                b_out.reshape(32, 128), ln2_gain.reshape(32, 128), ln2_bias.reshape(32, 128), w_up, b_up.reshape(32, 128), w_down, b_down.reshape(32, 128))
        hbm = pl.BlockSpec(memory_space=pltpu.HBM)
        dma = pltpu.SemaphoreType.DMA
        rs_buffers = [pltpu.VMEM((NC, 2, ROWS, PN), BF16), pltpu.VMEM((NC, 2, ROWS, PN), BF16), pltpu.VMEM((NC, ROWS, PN), BF16), pltpu.VMEM((NC, ROWS, PN), BF16)]
        result = pl.pallas_call(
            kernel,
            out_shape=pltpu.VMEM((ROWS, D), BF16),
            in_specs=[hbm] * len(args),
            out_specs=pl.BlockSpec(memory_space=pltpu.VMEM),
            scratch_shapes=[
                pltpu.VMEM((STAGES, STAGE_ROWS, 3, HEADS, HEAD_DIM), BF16),
                pltpu.VMEM((SLOTS, PK, PN), BF16),
                pltpu.VMEM((ROWS, D), BF16),
                pltpu.VMEM((4, ROWS, D), BF16),
                pltpu.VMEM((4, ROWS, D), BF16),
                pltpu.VMEM((TOKENS, FF), F32),
                pltpu.VMEM((TOKENS, QKV), BF16),
                pltpu.VMEM((TOKENS, HEADS * HEAD_DIM), BF16),
                pltpu.VMEM((TOKENS, FF), BF16),
                pltpu.VMEM((NC, 2, ROWS, PN), F32),
                pltpu.VMEM((4, ROWS, PN), F32),
                *rs_buffers,
                *rs_buffers,
                pltpu.VMEM((NC, ROWS, PN), F32),
                pltpu.VMEM((4, 8, 128), F32),
                pltpu.VMEM((4, ROWS, 128), F32),
                pltpu.VMEM((128, 128), F32),
                pltpu.VMEM((4, 32, 128), F32),
                pltpu.VMEM((3, 32, 128), BF16),
                pltpu.VMEM((3, HEADS, HEAD_DIM), BF16),
                pltpu.VMEM((7, 1, D), F32),
                pltpu.VMEM((1, QKV), F32),
                pltpu.VMEM((TOKENS, TOKENS), F32),
                dma((STAGES,)), dma((SLOTS,)), dma((8,)), dma((1,)),
                dma((3, KC)), dma((3, KC)), dma((3, KC)), dma((3, KC)), dma((3,)), dma((3,)),
                dma((2, NC)), dma((2, NC)), dma((2, NC)), dma((2, NC)),
            ],
            compiler_params=pltpu.CompilerParams(collective_id=0, has_side_effects=True, vmem_limit_bytes=62 * 2**20),
            name="decoder_layer",
        )(*args)
        return result.reshape(hidden.shape)

    in_layout = (P("dp", "tp", None), P(), P(), P(None, None, "tp", None), P(None, "tp", None), P("tp", None, None), P(), P(), P(), P(None, "tp"), P("tp"), P("tp", None), P())
    return jax.shard_map(device_body, mesh=mesh, in_specs=in_layout, out_specs=P("dp", "tp", None), check_vma=False)
```

```python
import jax
import jax.numpy as jnp
from jax import lax
from jax.experimental import pallas as pl
from jax.experimental.pallas import tpu as pltpu
from jax.sharding import PartitionSpec as P

MESH = pl.DeviceIdType.MESH
F32, BF16 = jnp.float32, jnp.bfloat16

LN_EPS = 1e-5
N_BATCH, BLOCK, D = 3, 16, 4096
ROWS = N_BATCH * BLOCK
TOKENS = 4 * ROWS
HEADS, HEAD_DIM = 8, 128
FF = 4096
QKV = 3 * HEADS * HEAD_DIM

PK, PN = 1024, 512
KC = D // PK
NC = D // PN
N_QKV, N_OUT, N_UP, N_DOWN = 24, 8, 32, 32
G_OUT, G_UP, G_DOWN = 24, 32, 64
SLOTS = 36
STAGE_ROWS, STAGES = 256, 4
STEPS = D // STAGE_ROWS


def kernel(x_hbm, g1_hbm, b1_hbm, wqkv_hbm, bqkv_hbm, wout_hbm, bout_hbm, g2_hbm, b2_hbm, wup_hbm, bup_hbm, wdown_hbm, bdown_hbm, out_ref,
           stage, slots, x_own, h_all, x1_all, acc, qkv_bf, ctx, u, own, pf,
           psend1, prec1, xsend1, xrec1, psend2, prec2, xsend2, xrec2, xsum, stats, stat_cols, square,
           vec_f32, vec_bf, bqkv_v, rows, bqkv_row, mask,
           stage_sem, slot_sem, small_sem, x_sem,
           ag_s, ag_r, ag2_s, ag2_r, st_s, st_r, rs1_s, rs1_r, rs2_s, rs2_r):
    dp = lax.axis_index("dp")
    me = lax.axis_index("tp")
    core = lax.rem(me, 2)
    chip = lax.div(me, 2)
    partner = me + 1 - 2 * core
    cross = lax.rem(me + 2, 4)
    far = lax.rem(partner + 2, 4)
    other_core = 1 - core
    other_chip = 1 - chip

    def stage_copy(i):
        return pltpu.make_async_copy(wqkv_hbm.at[pl.ds(i * STAGE_ROWS, STAGE_ROWS)], stage.at[lax.rem(i, STAGES)], stage_sem.at[lax.rem(i, STAGES)])

    def to_slot(src, g):
        s = lax.rem(g, SLOTS)
        return pltpu.make_async_copy(src, slots.at[s], slot_sem.at[s])

    def out_copy(n):
        return to_slot(wout_hbm.at[:, pl.ds(n * PN, PN)], G_OUT + n)

    def up_copy(i):
        k, n = lax.div(i, NC), lax.rem(i, NC)
        return to_slot(wup_hbm.at[pl.ds(pl.multiple_of(k * PK, PK), PK), pl.ds(pl.multiple_of(n * PN, PN), PN)], G_UP + i)

    def down_copy(i):
        n, k = lax.div(i, KC), lax.rem(i, KC)
        return to_slot(wdown_hbm.at[pl.ds(pl.multiple_of(k * PK, PK), PK), pl.ds(pl.multiple_of(n * PN, PN), PN)], G_DOWN + i)

    barrier = pltpu.get_barrier_semaphore()
    for peer in (partner, cross, far):
        pl.semaphore_signal(barrier, inc=1, device_id=(dp, peer), device_id_type=MESH)
    G1, B1, G2, B2, BOUT, BUP, BDOWN = range(7)
    x_copy = pltpu.make_async_copy(x_hbm, x_own, x_sem.at[0])
    smalls = [pltpu.make_async_copy(src, vec_f32.at[i], small_sem.at[i]) for i, src in enumerate((g1_hbm, b1_hbm, g2_hbm, b2_hbm))]
    smalls += [pltpu.make_async_copy(src, vec_bf.at[i], small_sem.at[4 + i]) for i, src in enumerate((bout_hbm, bup_hbm, bdown_hbm))]
    smalls += [pltpu.make_async_copy(bqkv_hbm, bqkv_v, small_sem.at[7])]
    smalls[G1].start()
    smalls[B1].start()
    x_copy.start()

    def f32_row(i):
        for j in range(32):
            rows[i, :, j * 128:(j + 1) * 128] = vec_f32[i, j:j + 1, :]

    def row_stats(x):
        mean = jnp.mean(x, axis=-1, keepdims=True)
        centered = x - mean
        var = jnp.mean(centered * centered, axis=-1, keepdims=True)
        return mean, lax.rsqrt(var + LN_EPS)

    for i in (G1, B1):
        smalls[i].wait()
        f32_row(i)
    x_copy.wait()
    for i in range(STAGES):
        stage_copy(i).start()
    for c in smalls[2:]:
        c.start()
    for b in range(N_BATCH):
        r = pl.ds(b * BLOCK, BLOCK)
        xf = x_own[r, :].astype(F32)
        mean, rstd = row_stats(xf)
        h_all[me, r, :] = ((xf - mean) * rstd * rows[G1] + rows[B1]).astype(BF16)

    pl.semaphore_wait(barrier, 3)

    def push(buf, block, c, width, s, r, which, peer):
        ref = buf.at[block, :, pl.ds(c * width, width)]
        return pltpu.make_async_remote_copy(src_ref=ref, dst_ref=ref, send_sem=s.at[which, c], recv_sem=r.at[which, c], device_id=(dp, peer), device_id_type=MESH)

    def ag1(which, block, peer, c):
        return push(h_all, block, c, PK, ag_s, ag_r, which, peer)

    for c in range(KC):
        ag1(0, me, cross, c).start()
    for c in range(KC):
        ag1(1, me, partner, c).start()

    def ag1_forward(c):
        ag1(0, cross, cross, c).wait_recv()
        ag1(2, cross, partner, c).start()

    def relayout(i):
        s = lax.rem(i, STAGES)
        k, off = lax.div(i, 4), lax.rem(i, 4)
        r = pl.ds(pl.multiple_of(off * STAGE_ROWS, STAGE_ROWS), STAGE_ROWS)
        for t in range(3):
            w = stage[s, :, t].reshape(STAGE_ROWS, HEADS * HEAD_DIM)
            slots[k * 6 + 2 * t, r, :] = w[:, :PN]
            slots[k * 6 + 2 * t + 1, r, :] = w[:, PN:]

    def relayout_step(i, carry):
        stage_copy(i).wait()
        relayout(i)

        @pl.when(i + STAGES < STEPS)
        def _():
            stage_copy(i + STAGES).start()

        return carry

    lax.fori_loop(0, STEPS - STAGES, relayout_step, 0)
    for n in range(N_OUT):
        out_copy(n).start()
    for i in range(SLOTS - G_UP):
        up_copy(i).start()
    for c in smalls[2:]:
        c.wait()
    for i in (G2, B2):
        f32_row(i)
    for i in range(3):
        vals = vec_bf[i].astype(F32)
        for j in range(32):
            rows[4 + i, :, j * 128:(j + 1) * 128] = vals[j:j + 1, :]
    for t in range(3):
        vals = bqkv_v[t].astype(F32)
        for j in range(HEADS):
            bqkv_row[:, (t * HEADS + j) * 128:(t * HEADS + j + 1) * 128] = vals[j:j + 1, :]

    def token_place(axis):
        t = lax.broadcasted_iota(jnp.int32, (TOKENS, TOKENS), axis)
        d = sum((t >= ROWS * i).astype(jnp.int32) for i in range(1, 4))
        t = t - ROWS * d
        b = sum((t >= BLOCK * i).astype(jnp.int32) for i in range(1, N_BATCH))
        return b, d * BLOCK + t - BLOCK * b

    (q_seq, q_pos), (k_seq, k_pos) = token_place(0), token_place(1)
    square[...] = jnp.zeros_like(square)
    mask[...] = ((q_seq == k_seq) & (q_pos >= k_pos)).astype(F32)

    ag1_forward(0)
    ag1_forward(1)
    lax.fori_loop(STEPS - STAGES, STEPS, relayout_step, 0)

    def tokens(buf, c):
        return buf[:, :, c * PK:(c + 1) * PK].reshape(TOKENS, PK)

    def qkv_chunk(c):
        ag1(1, partner, partner, c).wait_recv()
        ag1(2, far, partner, c).wait_recv()
        h = tokens(h_all, c)
        for n in range(6):
            cols = slice(n * PN, (n + 1) * PN)
            part = jnp.dot(h, slots[c * 6 + n], preferred_element_type=F32)
            if c:
                part = part + acc[:, cols]
            if c < KC - 1:
                acc[:, cols] = part
            else:
                qkv_bf[:, cols] = (part + bqkv_row[:, cols]).astype(BF16)
        for n in range(6):
            up_copy(c * 6 + n + SLOTS - G_UP).start()

    for c in range(KC):
        if 1 <= c < KC - 1:
            ag1_forward(c + 1)
        qkv_chunk(c)
    for c in range(KC):
        ag1(0, me, cross, c).wait_send()
        ag1(1, me, partner, c).wait_send()
        ag1(2, cross, partner, c).wait_send()

    keep = mask[...] > 0.5
    for first in range(0, HEADS, 4):
        heads = range(first, first + 4)

        def part_of(t, j):
            return qkv_bf[:, (t * HEADS + j) * HEAD_DIM:(t * HEADS + j + 1) * HEAD_DIM]

        logits = [lax.dot_general(part_of(0, j), part_of(1, j), (((1,), (1,)), ((), ())), preferred_element_type=F32) for j in heads]
        logits = [jnp.where(keep, x * HEAD_DIM ** -0.5, -1e30) for x in logits]
        tops = [jnp.max(x, axis=-1, keepdims=True) for x in logits]
        es = [jnp.exp(x - t) for x, t in zip(logits, tops)]
        sums = [jnp.sum(e, axis=-1, keepdims=True) for e in es]
        ps = [(e * (1.0 / z)).astype(BF16) for e, z in zip(es, sums)]
        for j, p in zip(heads, ps):
            ctx[:, j * HEAD_DIM:(j + 1) * HEAD_DIM] = jnp.dot(p, part_of(2, j), preferred_element_type=F32).astype(BF16)

    def rs_pair(psend, prec, s, r, n):
        return pltpu.make_async_remote_copy(src_ref=psend.at[n], dst_ref=prec.at[n], send_sem=s.at[0, n], recv_sem=r.at[0, n], device_id=(dp, partner), device_id_type=MESH)

    def rs_cross(xsend, xrec, s, r, n):
        return pltpu.make_async_remote_copy(src_ref=xsend.at[n], dst_ref=xrec.at[n], send_sem=s.at[1, n], recv_sem=r.at[1, n], device_id=(dp, cross), device_id_type=MESH)

    def rs_a(part, psend, prec, s, r, n):
        pf[...] = part.reshape(4, ROWS, PN)
        for q in range(2):
            psend[n, q] = pf[2 * q + other_core].astype(BF16)
            own[n, q] = pf[2 * q + core]
        rs_pair(psend, prec, s, r, n).start()

    def rs_b(psend, prec, xsend, xrec, s, r, n):
        rs_pair(psend, prec, s, r, n).wait_recv()
        xsend[n] = (own[n, other_chip] + prec[n, other_chip].astype(F32)).astype(BF16)
        rs_cross(xsend, xrec, s, r, n).start()
        xsum[n] = own[n, chip] + prec[n, chip].astype(F32)

    def rs_c(xsend, xrec, s, r, n):
        rs_cross(xsend, xrec, s, r, n).wait_recv()
        return xsum[n] + xrec[n].astype(F32)

    ctx_rows = ctx[...]

    def out_a(n):
        out_copy(n).wait()
        rs_a(jnp.dot(ctx_rows, slots[(G_OUT + n) % SLOTS], preferred_element_type=F32), psend1, prec1, rs1_s, rs1_r, n)
        g = G_OUT + n + SLOTS
        (up_copy(g - G_UP) if g < G_DOWN else down_copy(g - G_DOWN)).start()

    def out_b(n):
        rs_b(psend1, prec1, xsend1, xrec1, rs1_s, rs1_r, n)

    def ag2(which, block, peer, c):
        return push(x1_all, block, c, PK, ag2_s, ag2_r, which, peer)

    def st(which, block, peer):
        ref = stats.at[block]
        return pltpu.make_async_remote_copy(src_ref=ref, dst_ref=ref, send_sem=st_s.at[which], recv_sem=st_r.at[which], device_id=(dp, peer), device_id_type=MESH)

    lead = 3
    for n in range(NC):
        out_a(n)
        if n >= lead:
            out_b(n - lead)
    for n in range(NC - lead, NC):
        out_b(n)
    for n in range(NC):
        cols = slice(n * PN, (n + 1) * PN)
        total = rs_c(xsend1, xrec1, rs1_s, rs1_r, n)
        x1_all[me, :, cols] = (x_own[:, cols].astype(F32) + (total + rows[BOUT, :, cols])).astype(BF16)
        if n == 1:
            ag2(0, me, cross, 0).start()
            ag2(1, me, partner, 0).start()
    for b in range(N_BATCH):
        r = pl.ds(b * BLOCK, BLOCK)
        mean, rstd = row_stats(x1_all[me, r, :].astype(F32))
        lane = lax.broadcasted_iota(jnp.int32, (BLOCK, 128), 1)
        square[r, :] = jnp.where(lane == 0, mean, rstd)
    stats[me] = square[...].T[:8]
    st(0, me, cross).start()
    st(2, me, far).start()
    st(1, me, partner).start()
    for c in range(1, KC):
        ag2(0, me, cross, c).start()
        ag2(1, me, partner, c).start()

    def ag2_forward(c):
        ag2(0, cross, cross, c).wait_recv()
        ag2(2, cross, partner, c).start()

    def arrive(c):
        ag2(1, partner, partner, c).wait_recv()
        ag2(2, far, partner, c).wait_recv()

    def normalize(c):
        cols = slice(c * PK, (c + 1) * PK)
        for d in range(4):
            xf = x1_all[d, :, cols].astype(F32)
            h_all[d, :, cols] = ((xf - stat_cols[d, :, 0:1]) * stat_cols[d, :, 1:2] * rows[G2, :, cols] + rows[B2, :, cols]).astype(BF16)

    def up_panels(c, panels):
        for n in panels:
            up_copy(c * NC + n).wait()
        h = tokens(h_all, c)
        for n in panels:
            wide = slice(n * PN, (n + 1) * PN)
            part = jnp.dot(h, slots[(G_UP + c * NC + n) % SLOTS], preferred_element_type=F32)
            if c:
                part = part + acc[:, wide]
            if c < KC - 1:
                acc[:, wide] = part
            else:
                u[:, wide] = jax.nn.gelu(part + rows[BUP, :, wide], approximate=True).astype(BF16)

    def refill(c, panels):
        for n in panels:
            i = c * NC + n + G_UP + SLOTS - G_DOWN
            if i < N_DOWN:
                down_copy(i).start()

    ag2_forward(0)
    st(1, partner, partner).wait_recv()
    st(0, cross, cross).wait_recv()
    st(2, far, far).wait_recv()
    for d in range(4):
        square[0:8, :] = stats[d]
        stat_cols[d] = square[...].T[:ROWS]
    arrive(0)
    normalize(0)
    for c in range(KC):
        up_panels(c, range(0, 3))
        refill(c, range(0, 3))
        if c < KC - 1:
            ag2_forward(c + 1)
        up_panels(c, range(3, 7))
        refill(c, range(3, 7))
        if c < KC - 1:
            arrive(c + 1)
        up_panels(c, range(7, 8))
        if c < KC - 1:
            normalize(c + 1)
        refill(c, range(7, 8))

    def down_a(n):
        for k in range(KC):
            down_copy(n * KC + k).wait()
        part = None
        for k in range(KC):
            term = jnp.dot(u[:, k * PK:(k + 1) * PK], slots[(G_DOWN + n * KC + k) % SLOTS], preferred_element_type=F32)
            part = term if part is None else part + term
        rs_a(part, psend2, prec2, rs2_s, rs2_r, n)

    def down_b(n):
        rs_b(psend2, prec2, xsend2, xrec2, rs2_s, rs2_r, n)

    def down_c(n):
        cols = slice(n * PN, (n + 1) * PN)
        total = rs_c(xsend2, xrec2, rs2_s, rs2_r, n)
        out_ref[:, cols] = (x1_all[me, :, cols].astype(F32) + (total + rows[BDOWN, :, cols])).astype(BF16)

    for n in range(NC):
        down_a(n)
        if n >= 1:
            down_b(n - 1)
    down_b(NC - 1)
    for n in range(NC):
        down_c(n)

    for n in range(NC):
        rs_pair(psend1, prec1, rs1_s, rs1_r, n).wait_send()
        rs_cross(xsend1, xrec1, rs1_s, rs1_r, n).wait_send()
        rs_pair(psend2, prec2, rs2_s, rs2_r, n).wait_send()
        rs_cross(xsend2, xrec2, rs2_s, rs2_r, n).wait_send()
    for c in range(KC):
        ag2(0, me, cross, c).wait_send()
        ag2(1, me, partner, c).wait_send()
        ag2(2, cross, partner, c).wait_send()
    st(0, me, cross).wait_send()
    st(1, me, partner).wait_send()
    st(2, me, far).wait_send()


def solution(mesh):
    def device_body(hidden, ln1_gain, ln1_bias, w_qkv, b_qkv, w_out, b_out, ln2_gain, ln2_bias, w_up, b_up, w_down, b_down):
        args = (hidden.reshape(ROWS, D), ln1_gain.reshape(32, 128), ln1_bias.reshape(32, 128), w_qkv, b_qkv, w_out.reshape(HEADS * HEAD_DIM, D),
                b_out.reshape(32, 128), ln2_gain.reshape(32, 128), ln2_bias.reshape(32, 128), w_up, b_up.reshape(32, 128), w_down, b_down.reshape(32, 128))
        hbm = pl.BlockSpec(memory_space=pltpu.HBM)
        dma = pltpu.SemaphoreType.DMA
        rs_buffers = [pltpu.VMEM((NC, 2, ROWS, PN), BF16), pltpu.VMEM((NC, 2, ROWS, PN), BF16), pltpu.VMEM((NC, ROWS, PN), BF16), pltpu.VMEM((NC, ROWS, PN), BF16)]
        result = pl.pallas_call(
            kernel,
            out_shape=pltpu.VMEM((ROWS, D), BF16),
            in_specs=[hbm] * len(args),
            out_specs=pl.BlockSpec(memory_space=pltpu.VMEM),
            scratch_shapes=[
                pltpu.VMEM((STAGES, STAGE_ROWS, 3, HEADS, HEAD_DIM), BF16),
                pltpu.VMEM((SLOTS, PK, PN), BF16),
                pltpu.VMEM((ROWS, D), BF16),
                pltpu.VMEM((4, ROWS, D), BF16),
                pltpu.VMEM((4, ROWS, D), BF16),
                pltpu.VMEM((TOKENS, FF), F32),
                pltpu.VMEM((TOKENS, QKV), BF16),
                pltpu.VMEM((TOKENS, HEADS * HEAD_DIM), BF16),
                pltpu.VMEM((TOKENS, FF), BF16),
                pltpu.VMEM((NC, 2, ROWS, PN), F32),
                pltpu.VMEM((4, ROWS, PN), F32),
                *rs_buffers,
                *rs_buffers,
                pltpu.VMEM((NC, ROWS, PN), F32),
                pltpu.VMEM((4, 8, 128), F32),
                pltpu.VMEM((4, ROWS, 128), F32),
                pltpu.VMEM((128, 128), F32),
                pltpu.VMEM((4, 32, 128), F32),
                pltpu.VMEM((3, 32, 128), BF16),
                pltpu.VMEM((3, HEADS, HEAD_DIM), BF16),
                pltpu.VMEM((7, 1, D), F32),
                pltpu.VMEM((1, QKV), F32),
                pltpu.VMEM((TOKENS, TOKENS), F32),
                dma((STAGES,)), dma((SLOTS,)), dma((8,)), dma((1,)),
                dma((3, KC)), dma((3, KC)), dma((3, KC)), dma((3, KC)), dma((3,)), dma((3,)),
                dma((2, NC)), dma((2, NC)), dma((2, NC)), dma((2, NC)),
            ],
            compiler_params=pltpu.CompilerParams(collective_id=0, has_side_effects=True, vmem_limit_bytes=62 * 2**20),
            name="decoder_layer",
        )(*args)
        return result.reshape(hidden.shape)

    in_layout = (P("dp", "tp", None), P(), P(), P(None, None, "tp", None), P(None, "tp", None), P("tp", None, None), P(), P(), P(), P(None, "tp"), P("tp"), P("tp", None), P())
    return jax.shard_map(device_body, mesh=mesh, in_specs=in_layout, out_specs=P("dp", "tp", None), check_vma=False)
```

```python
import math

import jax
import jax.numpy as jnp
from jax import lax
from jax.experimental import pallas as pl
from jax.experimental.pallas import tpu as pltpu
from jax.sharding import PartitionSpec as P

MESH = pl.DeviceIdType.MESH
F32, BF16 = jnp.float32, jnp.bfloat16

LN_EPS = 1e-5
N_BATCH, BLOCK, D = 3, 16, 4096
ROWS = N_BATCH * BLOCK
TOKENS = 4 * ROWS
HEADS, HEAD_DIM = 8, 128
FF = 4096
QKV = 3 * HEADS * HEAD_DIM

PK, PN = 1024, 512
NK, NN = D // PK, D // PN
AG1_CHUNKS = [(k * PK, PK) for k in range(NK)]
AG2_CHUNKS = [(0, 1024), (1024, 1024), (2048, 1024), (3072, 512), (3584, 512)]
RS_CHUNKS = [(n * PN, PN) for n in range(NN)]
RING = 9
G_OUT, G_UP, G_DOWN, G_END = 6, 8, 16, 24
STAGE_ROWS, STAGES = 256, 4
STEPS = D // STAGE_ROWS


def kernel(x_hbm, g1_hbm, b1_hbm, wqkv_hbm, bqkv_hbm, wout_hbm, bout_hbm, g2_hbm, b2_hbm, wup_hbm, bup_hbm, wdown_hbm, bdown_hbm, out_ref,
           stage, x_own, h_all, x1_all, h2_even, h2_odd, acc, qkv_bf, ctx, u,
           psend1, prec1, xsend1, xrec1, psend2, prec2, xsend2, xrec2, stats, stat_cols, square,
           vec_f32, vec_bf, bqkv_v, rows, bqkv_row, mask,
           stage_sem, ring_sem, small_sem, send_sem, gather_sem, st_sem, rs_sem, *ring):
    dp = lax.axis_index("dp")
    me = lax.axis_index("tp")
    core = lax.rem(me, 2)
    chip = lax.div(me, 2)
    partner = me + 1 - 2 * core
    cross = lax.rem(me + 2, 4)
    far = lax.rem(partner + 2, 4)
    other_core = 1 - core
    other_chip = 1 - chip
    SEND_AG1, SEND_AG2, SEND_ST, SEND_RS1, SEND_RS2 = 0, 1, 2, 3, 5

    def remote(src, dst, send, recv, peer):
        return pltpu.make_async_remote_copy(src_ref=src, dst_ref=dst, send_sem=send, recv_sem=recv, device_id=(dp, peer), device_id_type=MESH)

    def stage_copy(i):
        return pltpu.make_async_copy(wqkv_hbm.at[pl.ds(i * STAGE_ROWS, STAGE_ROWS)], stage.at[lax.rem(i, STAGES)], stage_sem.at[lax.rem(i, STAGES)])

    def load_group(g):
        to, sem = ring[g % RING], ring_sem.at[g % RING]
        if g >= G_END:
            return
        if g >= G_DOWN:
            pltpu.make_async_copy(wdown_hbm.at[:, :, pl.ds((g - G_DOWN) * PN, PN)], to, sem).start()
            return
        for m in range(4):
            if g >= G_UP:
                k, n = (g - G_UP) // 2, (g - G_UP) % 2 * 4 + m
                src = wup_hbm.at[pl.ds(k * PK, PK), pl.ds(n * PN, PN)]
            else:
                src = wout_hbm.at[:, pl.ds(((g - G_OUT) * 4 + m) * PN, PN)]
            pltpu.make_async_copy(src, to.at[m], sem).start()

    def await_group(g):
        pltpu.make_async_copy(wdown_hbm.at[:, :, pl.ds(0, PN)], ring[g % RING], ring_sem.at[g % RING]).wait()

    barrier = pltpu.get_barrier_semaphore()
    for peer in (partner, cross, far):
        pl.semaphore_signal(barrier, inc=1, device_id=(dp, peer), device_id_type=MESH)
    G1, B1, G2, B2, BOUT, BUP, BDOWN = range(7)
    x_copy = pltpu.make_async_copy(x_hbm, x_own, small_sem.at[4])
    for i, src in enumerate((g1_hbm, b1_hbm)):
        pltpu.make_async_copy(src, vec_f32.at[i], small_sem.at[0]).start()
    x_copy.start()
    stage_copy(0).start()

    def f32_row(i):
        for j in range(32):
            rows[i, :, j * 128:(j + 1) * 128] = vec_f32[i, j:j + 1, :]

    def row_stats(x):
        mean = jnp.mean(x, axis=-1, keepdims=True)
        centered = x - mean
        var = jnp.mean(centered * centered, axis=-1, keepdims=True)
        return mean, lax.rsqrt(var + LN_EPS)

    pltpu.make_async_copy(vec_f32.at[pl.ds(2, 2)], vec_f32.at[pl.ds(0, 2)], small_sem.at[0]).wait()
    for i in (G1, B1):
        f32_row(i)
    x_copy.wait()
    for i in range(1, STAGES):
        stage_copy(i).start()
    for i, src in enumerate((g2_hbm, b2_hbm)):
        pltpu.make_async_copy(src, vec_f32.at[2 + i], small_sem.at[1]).start()
    for i, src in enumerate((bout_hbm, bup_hbm, bdown_hbm)):
        pltpu.make_async_copy(src, vec_bf.at[i], small_sem.at[2]).start()
    bqkv_copy = pltpu.make_async_copy(bqkv_hbm, bqkv_v, small_sem.at[3])
    bqkv_copy.start()
    for b in range(N_BATCH):
        r = pl.ds(b * BLOCK, BLOCK)
        xf = x_own[r, :].astype(F32)
        mean, rstd = row_stats(xf)
        h_all[me, r, :] = ((xf - mean) * rstd * rows[G1] + rows[B1]).astype(BF16)

    pl.semaphore_wait(barrier, 3)

    PARTNER, CROSS, FAR = range(3)

    def push(buf, chunks, send, which, block, peer, c):
        ref = buf.at[block, :, pl.ds(*chunks[c])]
        return remote(ref, ref, send_sem.at[send], gather_sem.at[which, c], peer)

    def ag1(which, block, peer, c):
        return push(h_all, AG1_CHUNKS, SEND_AG1, which, block, peer, c)

    def ag1_partner(block):
        return remote(h_all.at[block], h_all.at[block], send_sem.at[SEND_AG1], gather_sem.at[PARTNER, 0], partner)

    for c in range(NK):
        ag1(CROSS, me, cross, c).start()
    ag1_partner(me).start()

    def ag1_forward(c):
        ag1(CROSS, cross, cross, c).wait_recv()
        ag1(FAR, cross, partner, c).start()

    def relayout(k, off):
        s = lax.rem(k * 4 + off, STAGES)
        r = pl.ds(pl.multiple_of(off * STAGE_ROWS, STAGE_ROWS), STAGE_ROWS)
        for t in range(3):
            w = stage[s, :, t].reshape(STAGE_ROWS, HEADS * HEAD_DIM)
            for half in range(2):
                p = k * 6 + 2 * t + half
                ring[p // 4][p % 4, r, :] = w[:, half * PN:(half + 1) * PN]

    def relayout_chunk(k):
        def step(off, carry):
            stage_copy(k * 4 + off).wait()
            relayout(k, off)
            if k < NK - 1:
                stage_copy(k * 4 + off + STAGES).start()
            return carry

        lax.fori_loop(0, 4, step, 0)

    for k in range(3):
        relayout_chunk(k)
    pltpu.make_async_copy(vec_f32.at[pl.ds(0, 2)], vec_f32.at[pl.ds(2, 2)], small_sem.at[1]).wait()
    pltpu.make_async_copy(vec_bf, vec_bf, small_sem.at[2]).wait()
    bqkv_copy.wait()
    for i in (G2, B2):
        f32_row(i)
    for i in range(3):
        vals = vec_bf[i].astype(F32)
        for j in range(32):
            rows[4 + i, :, j * 128:(j + 1) * 128] = vals[j:j + 1, :]
    for t in range(3):
        vals = bqkv_v[t].astype(F32)
        for j in range(HEADS):
            bqkv_row[:, (t * HEADS + j) * 128:(t * HEADS + j + 1) * 128] = vals[j:j + 1, :]

    def token_place(axis):
        t = lax.broadcasted_iota(jnp.int32, (TOKENS, TOKENS), axis)
        d = sum((t >= ROWS * i).astype(jnp.int32) for i in range(1, 4))
        t = t - ROWS * d
        b = sum((t >= BLOCK * i).astype(jnp.int32) for i in range(1, N_BATCH))
        return b, d * BLOCK + t - BLOCK * b

    (q_seq, q_pos), (k_seq, k_pos) = token_place(0), token_place(1)
    square[...] = jnp.zeros_like(square)
    mask[...] = ((q_seq == k_seq) & (q_pos >= k_pos)).astype(F32)
    ag1_forward(0)
    ag1_forward(1)
    relayout_chunk(3)
    for g in range(G_OUT, RING):
        load_group(g)
    def all_rows(ref, start, size):
        return ref[:, :, start:start + size].reshape(TOKENS, size)

    def qkv_chunk(c):
        ag1(FAR, far, partner, c).wait_recv()
        h = all_rows(h_all, *AG1_CHUNKS[c])
        for n in range(6):
            p = c * 6 + n
            part = jnp.dot(h, ring[p // 4][p % 4], preferred_element_type=F32)
            if c:
                part = part + all_rows(acc, n * PN, PN)
            if c < NK - 1:
                acc[:, :, n * PN:(n + 1) * PN] = part.reshape(4, ROWS, PN)
            else:
                qkv_bf[:, n * PN:(n + 1) * PN] = (part + bqkv_row[:, n * PN:(n + 1) * PN]).astype(BF16)
        for g in range(c * 6 // 4, (c + 1) * 6 // 4):
            load_group(g + RING)

    ag1_partner(partner).wait_recv()
    for c in range(NK):
        if c + 2 < NK:
            ag1_forward(c + 2)
        qkv_chunk(c)

    keep = mask[...] > 0.5
    for first in range(0, HEADS, 4):
        heads = range(first, first + 4)

        def part_of(t, j):
            return qkv_bf[:, (t * HEADS + j) * HEAD_DIM:(t * HEADS + j + 1) * HEAD_DIM]

        logits = [lax.dot_general(part_of(0, j), part_of(1, j), (((1,), (1,)), ((), ())), preferred_element_type=F32) for j in heads]
        logits = [jnp.where(keep, x * HEAD_DIM ** -0.5, -1e30) for x in logits]
        tops = [jnp.max(x, axis=-1, keepdims=True) for x in logits]
        es = [jnp.exp(x - t) for x, t in zip(logits, tops)]
        sums = [jnp.sum(e, axis=-1, keepdims=True) for e in es]
        ps = [(e * (1.0 / z)).astype(BF16) for e, z in zip(es, sums)]
        for j, p in zip(heads, ps):
            ctx[:, j * HEAD_DIM:(j + 1) * HEAD_DIM] = jnp.dot(p, part_of(2, j), preferred_element_type=F32).astype(BF16)

    def reduction(psend, prec, xsend, xrec, send):
        def pair(n):
            at = (slice(None), slice(None), pl.ds(*RS_CHUNKS[n]))
            return remote(psend.at[at], prec.at[at], send_sem.at[send], rs_sem.at[0, n], partner)

        def across(n):
            at = (slice(None), pl.ds(*RS_CHUNKS[n]))
            return remote(xsend.at[at], xrec.at[at], send_sem.at[send + 1], rs_sem.at[1, n], cross)

        def to_pair(n, part):
            cols = pl.ds(*RS_CHUNKS[n])
            acc[:, :, cols] = part.reshape(4, ROWS, RS_CHUNKS[n][1])
            for q in range(2):
                psend[q, :, cols] = acc[2 * q + other_core, :, cols].astype(BF16)
            pair(n).start()

        def to_cross(n):
            cols = pl.ds(*RS_CHUNKS[n])
            pair(n).wait_recv()
            xsend[:, cols] = (acc[2 * other_chip + core, :, cols] + prec[other_chip, :, cols].astype(F32)).astype(BF16)
            across(n).start()

        def total(n):
            cols = pl.ds(*RS_CHUNKS[n])
            across(n).wait_recv()
            return acc[me, :, cols] + prec[chip, :, cols].astype(F32) + xrec[:, cols].astype(F32)

        def drain():
            remote(psend, prec, send_sem.at[send], rs_sem.at[0, 0], partner).wait_send()
            remote(xsend, xrec, send_sem.at[send + 1], rs_sem.at[1, 0], cross).wait_send()

        return to_pair, to_cross, total, drain

    NR = len(RS_CHUNKS)
    rs1_pair, rs1_cross, rs1_total, rs1_drain = reduction(psend1, prec1, xsend1, xrec1, SEND_RS1)
    rs2_pair, rs2_cross, rs2_total, rs2_drain = reduction(psend2, prec2, xsend2, xrec2, SEND_RS2)

    def ag2(which, block, peer, c):
        return push(x1_all, AG2_CHUNKS, SEND_AG2, which, block, peer, c)

    def st(block, peer):
        return remote(stats.at[block], stats.at[block], send_sem.at[SEND_ST], st_sem.at[0], peer)

    ctx_rows = ctx[...]
    lead = 2
    for g in range(G_OUT, G_UP):
        await_group(g)
    for n, (start, size) in enumerate(RS_CHUNKS):
        g, m = G_OUT + start // PN // 4, start // PN % 4
        rs1_pair(n, jnp.dot(ctx_rows, ring[g % RING][m, :, start % PN:start % PN + size], preferred_element_type=F32))
        if n >= lead:
            rs1_cross(n - lead)
    for g in range(G_OUT, G_UP):
        load_group(g + RING)
    for n in range(NR - lead, NR):
        rs1_cross(n)
    for n, (start, size) in enumerate(RS_CHUNKS):
        cols = pl.ds(start, size)
        x1_all[me, :, cols] = (x_own[:, cols].astype(F32) + (rs1_total(n) + rows[BOUT, :, cols])).astype(BF16)
        if start + size == sum(AG2_CHUNKS[0]):
            ag2(CROSS, me, cross, 0).start()
            ag2(PARTNER, me, partner, 0).start()
    for b in range(N_BATCH):
        r = pl.ds(b * BLOCK, BLOCK)
        mean, rstd = row_stats(x1_all[me, r, :].astype(F32))
        lane = lax.broadcasted_iota(jnp.int32, (BLOCK, 128), 1)
        square[r, :] = jnp.where(lane == 0, mean, rstd)
    stats[me] = square[...].T[:8]
    for peer in (cross, far, partner):
        st(me, peer).start()
    for c in range(1, len(AG2_CHUNKS)):
        ag2(CROSS, me, cross, c).start()
        ag2(PARTNER, me, partner, c).start()

    def ag2_forward(c):
        ag2(CROSS, cross, cross, c).wait_recv()
        ag2(FAR, cross, partner, c).start()

    def normalize(c, blocks):
        start, size = AG2_CHUNKS[c]
        cols = pl.ds(start, size)
        to = (h2_even, h2_odd)[c % 2]
        for d in blocks:
            xf = x1_all[d, :, cols].astype(F32)
            to[d, :, 0:size] = ((xf - stat_cols[d, :, 0:1]) * stat_cols[d, :, 1:2] * rows[G2, :, cols] + rows[B2, :, cols]).astype(BF16)

    def gelu(x):
        scale = (2 / math.pi) ** 0.5
        halved = 0.5 * x
        return halved + halved * jnp.tanh(x * (scale + (scale * 0.044715) * (x * x)))

    def up_half(c, half):
        start, size = AG2_CHUNKS[c]
        h = all_rows((h2_even, h2_odd)[c % 2], 0, size)
        g = G_UP + start // PK * 2 + half
        for m in range(4):
            n = half * 4 + m
            part = jnp.dot(h, ring[g % RING][m, start % PK:start % PK + size, :], preferred_element_type=F32)
            part = part + (all_rows(acc, n * PN, PN) if c else rows[BUP, :, n * PN:(n + 1) * PN])
            if c < len(AG2_CHUNKS) - 1:
                acc[:, :, n * PN:(n + 1) * PN] = part.reshape(4, ROWS, PN)
            else:
                u[:, n * PN:(n + 1) * PN] = gelu(part).astype(BF16)

    def down_sum(n):
        total = None
        for k in range(NK):
            term = jnp.dot(u[:, k * PK:(k + 1) * PK], ring[(G_DOWN + n) % RING][k], preferred_element_type=F32)
            total = term if total is None else total + term
        return total

    ag2_forward(0)
    remote(stats.at[pl.ds(0, 3)], stats.at[pl.ds(0, 3)], send_sem.at[SEND_ST], st_sem.at[0], partner).wait_recv()
    for d in range(4):
        square[0:8, :] = stats[d]
        stat_cols[d] = square[...].T[:ROWS]
    ag2(PARTNER, partner, partner, 0).wait_recv()
    ag2(FAR, far, partner, 0).wait_recv()
    normalize(0, range(4))
    for c, (start, size) in enumerate(AG2_CHUNKS[:-1]):
        g = G_UP + start // PK * 2
        if start % PK == 0:
            await_group(g)
            await_group(g + 1)
        up_half(c, 0)
        ag2_forward(c + 1)
        ag2(PARTNER, partner, partner, c + 1).wait_recv()
        normalize(c + 1, (me, partner, cross))
        up_half(c, 1)
        if (start + size) % PK == 0:
            load_group(g + RING)
            load_group(g + 1 + RING)
        ag2(FAR, far, partner, c + 1).wait_recv()
        normalize(c + 1, (far,))

    await_group(G_DOWN)
    for half in range(2):
        up_half(len(AG2_CHUNKS) - 1, half)
    rs2_pair(0, down_sum(0))
    load_group(G_DOWN - 2 + RING)
    load_group(G_DOWN - 1 + RING)
    for n in range(1, NR):
        await_group(G_DOWN + n)
        rs2_pair(n, down_sum(n))
        rs2_cross(n - 1)
    rs2_cross(NR - 1)
    for n, (start, size) in enumerate(RS_CHUNKS):
        cols = pl.ds(start, size)
        out_ref[:, cols] = (x1_all[me, :, cols].astype(F32) + (rs2_total(n) + rows[BDOWN, :, cols])).astype(BF16)

    for buf, send in ((h_all, SEND_AG1), (x1_all, SEND_AG2), (stats, SEND_ST)):
        remote(buf.at[pl.ds(0, 3)], buf.at[pl.ds(0, 3)], send_sem.at[send], st_sem.at[0], partner).wait_send()
    rs1_drain()
    rs2_drain()


def solution(mesh):
    def device_body(hidden, ln1_gain, ln1_bias, w_qkv, b_qkv, w_out, b_out, ln2_gain, ln2_bias, w_up, b_up, w_down, b_down):
        args = (hidden.reshape(ROWS, D), ln1_gain.reshape(32, 128), ln1_bias.reshape(32, 128), w_qkv, b_qkv, w_out.reshape(HEADS * HEAD_DIM, D),
                b_out.reshape(32, 128), ln2_gain.reshape(32, 128), ln2_bias.reshape(32, 128), w_up, b_up.reshape(32, 128), w_down.reshape(NK, PK, D), b_down.reshape(32, 128))
        hbm = pl.BlockSpec(memory_space=pltpu.HBM)
        dma = pltpu.SemaphoreType.DMA
        rs_buffers = [pltpu.VMEM((2, ROWS, D), BF16), pltpu.VMEM((2, ROWS, D), BF16), pltpu.VMEM((ROWS, D), BF16), pltpu.VMEM((ROWS, D), BF16)]
        result = pl.pallas_call(
            kernel,
            out_shape=pltpu.VMEM((ROWS, D), BF16),
            in_specs=[hbm] * len(args),
            out_specs=pl.BlockSpec(memory_space=pltpu.VMEM),
            scratch_shapes=[
                pltpu.VMEM((STAGES, STAGE_ROWS, 3, HEADS, HEAD_DIM), BF16),
                pltpu.VMEM((ROWS, D), BF16),
                pltpu.VMEM((4, ROWS, D), BF16),
                pltpu.VMEM((4, ROWS, D), BF16),
                pltpu.VMEM((4, ROWS, PK), BF16),
                pltpu.VMEM((4, ROWS, PK), BF16),
                pltpu.VMEM((4, ROWS, FF), F32),
                pltpu.VMEM((TOKENS, QKV), BF16),
                pltpu.VMEM((TOKENS, HEADS * HEAD_DIM), BF16),
                pltpu.VMEM((TOKENS, FF), BF16),
                *rs_buffers,
                *rs_buffers,
                pltpu.VMEM((4, 8, 128), F32),
                pltpu.VMEM((4, ROWS, 128), F32),
                pltpu.VMEM((128, 128), F32),
                pltpu.VMEM((4, 32, 128), F32),
                pltpu.VMEM((3, 32, 128), BF16),
                pltpu.VMEM((3, HEADS, HEAD_DIM), BF16),
                pltpu.VMEM((7, 1, D), F32),
                pltpu.VMEM((1, QKV), F32),
                pltpu.VMEM((TOKENS, TOKENS), F32),
                dma((STAGES,)), dma((RING,)), dma((5,)), dma((7,)), dma((3, len(AG2_CHUNKS))), dma((1,)), dma((2, len(RS_CHUNKS))),
                *[pltpu.VMEM((4, PK, PN), BF16)] * RING,
            ],
            compiler_params=pltpu.CompilerParams(collective_id=0, has_side_effects=True, vmem_limit_bytes=62 * 2**20),
            name="decoder_layer",
        )(*args)
        return result.reshape(hidden.shape)

    in_layout = (P("dp", "tp", None), P(), P(), P(None, None, "tp", None), P(None, "tp", None), P("tp", None, None), P(), P(), P(), P(None, "tp"), P("tp"), P("tp", None), P())
    return jax.shard_map(device_body, mesh=mesh, in_specs=in_layout, out_specs=P("dp", "tp", None), check_vma=False)
```

```python
import math

import jax
import jax.numpy as jnp
from jax import lax
from jax.experimental import pallas as pl
from jax.experimental.pallas import tpu as pltpu
from jax.sharding import PartitionSpec as P

MESH = pl.DeviceIdType.MESH
F32, BF16 = jnp.float32, jnp.bfloat16

LN_EPS = 1e-5
N_BATCH, BLOCK, D = 3, 16, 4096
ROWS = N_BATCH * BLOCK
TOKENS = 4 * ROWS
HEADS, HEAD_DIM = 8, 128
FF = 4096
QKV = 3 * HEADS * HEAD_DIM

PK, PN = 1024, 512
NK, NN = D // PK, D // PN
AG1_CHUNKS = [(k * PK, PK) for k in range(NK)]
AG2_CHUNKS = [(0, 1024), (1024, 512), (1536, 1024), (2560, 1024), (3584, 512)]
RS_CHUNKS = [(n * PN, PN) for n in range(NN)]
RING = 9
G_OUT, G_UP, G_DOWN, G_END = 6, 8, 16, 24
STAGE_ROWS, STAGES = 256, 4
STEPS = D // STAGE_ROWS


def kernel(x_hbm, g1_hbm, b1_hbm, wqkv_hbm, bqkv_hbm, wout_hbm, bout_hbm, g2_hbm, b2_hbm, wup_hbm, bup_hbm, wdown_hbm, bdown_hbm, out_ref,
           stage, x_own, h_all, x1_all, h2_even, h2_odd, acc, qkv_bf, ctx, u,
           psend1, prec1, xsend1, xrec1, psend2, prec2, xsend2, xrec2, stats, stat_cols, square,
           vec_f32, vec_bf, bqkv_v, rows, bqkv_row, mask,
           stage_sem, ring_sem, small_sem, send_sem, gather_sem, st_sem, rs_sem, *ring):
    dp = lax.axis_index("dp")
    me = lax.axis_index("tp")
    core = lax.rem(me, 2)
    chip = lax.div(me, 2)
    partner = me + 1 - 2 * core
    cross = lax.rem(me + 2, 4)
    far = lax.rem(partner + 2, 4)
    other_core = 1 - core
    other_chip = 1 - chip
    SEND_AG1, SEND_AG2, SEND_ST, SEND_RS1, SEND_RS2 = 0, 1, 2, 3, 5

    def remote(src, dst, send, recv, peer):
        return pltpu.make_async_remote_copy(src_ref=src, dst_ref=dst, send_sem=send, recv_sem=recv, device_id=(dp, peer), device_id_type=MESH)

    def stage_copy(i):
        return pltpu.make_async_copy(wqkv_hbm.at[pl.ds(i * STAGE_ROWS, STAGE_ROWS)], stage.at[lax.rem(i, STAGES)], stage_sem.at[lax.rem(i, STAGES)])

    def load_group(g):
        to, sem = ring[g % RING], ring_sem.at[g % RING]
        if g >= G_END:
            return
        if g >= G_DOWN:
            pltpu.make_async_copy(wdown_hbm.at[:, :, pl.ds((g - G_DOWN) * PN, PN)], to, sem).start()
            return
        for m in range(4):
            if g >= G_UP:
                k, n = (g - G_UP) // 2, (g - G_UP) % 2 * 4 + m
                src = wup_hbm.at[pl.ds(k * PK, PK), pl.ds(n * PN, PN)]
            else:
                src = wout_hbm.at[:, pl.ds(((g - G_OUT) * 4 + m) * PN, PN)]
            pltpu.make_async_copy(src, to.at[m], sem).start()

    def await_group(g):
        pltpu.make_async_copy(wdown_hbm.at[:, :, pl.ds(0, PN)], ring[g % RING], ring_sem.at[g % RING]).wait()

    barrier = pltpu.get_barrier_semaphore()
    for peer in (partner, cross, far):
        pl.semaphore_signal(barrier, inc=1, device_id=(dp, peer), device_id_type=MESH)
    G1, B1, G2, B2, BOUT, BUP, BDOWN = range(7)
    x_copy = pltpu.make_async_copy(x_hbm, x_own, small_sem.at[4])
    for i, src in enumerate((g1_hbm, b1_hbm)):
        pltpu.make_async_copy(src, vec_f32.at[i], small_sem.at[0]).start()
    x_copy.start()
    stage_copy(0).start()

    def f32_row(i):
        for j in range(32):
            rows[i, :, j * 128:(j + 1) * 128] = vec_f32[i, j:j + 1, :]

    def row_stats(x):
        mean = jnp.mean(x, axis=-1, keepdims=True)
        centered = x - mean
        var = jnp.mean(centered * centered, axis=-1, keepdims=True)
        return mean, lax.rsqrt(var + LN_EPS)

    pltpu.make_async_copy(vec_f32.at[pl.ds(2, 2)], vec_f32.at[pl.ds(0, 2)], small_sem.at[0]).wait()
    for i in (G1, B1):
        f32_row(i)
    stage_copy(1).start()
    x_copy.wait()
    for i in range(2, STAGES):
        stage_copy(i).start()
    for i, src in enumerate((g2_hbm, b2_hbm)):
        pltpu.make_async_copy(src, vec_f32.at[2 + i], small_sem.at[1]).start()
    for i, src in enumerate((bout_hbm, bup_hbm, bdown_hbm)):
        pltpu.make_async_copy(src, vec_bf.at[i], small_sem.at[2]).start()
    bqkv_copy = pltpu.make_async_copy(bqkv_hbm, bqkv_v, small_sem.at[3])
    bqkv_copy.start()
    for b in range(N_BATCH):
        r = pl.ds(b * BLOCK, BLOCK)
        xf = x_own[r, :].astype(F32)
        mean, rstd = row_stats(xf)
        h_all[me, r, :] = ((xf - mean) * rstd * rows[G1] + rows[B1]).astype(BF16)

    pl.semaphore_wait(barrier, 3)

    PARTNER, CROSS, FAR = range(3)

    def push(buf, chunks, send, which, block, peer, c):
        ref = buf.at[block, :, pl.ds(*chunks[c])]
        return remote(ref, ref, send_sem.at[send], gather_sem.at[which, c], peer)

    def ag1(which, block, peer, c):
        return push(h_all, AG1_CHUNKS, SEND_AG1, which, block, peer, c)

    def ag1_partner(block):
        return remote(h_all.at[block], h_all.at[block], send_sem.at[SEND_AG1], gather_sem.at[PARTNER, 0], partner)

    for c in range(NK):
        ag1(CROSS, me, cross, c).start()
    ag1_partner(me).start()

    def ag1_forward(c):
        ag1(CROSS, cross, cross, c).wait_recv()
        ag1(FAR, cross, partner, c).start()

    def relayout(k, off):
        s = lax.rem(k * 4 + off, STAGES)
        r = pl.ds(pl.multiple_of(off * STAGE_ROWS, STAGE_ROWS), STAGE_ROWS)
        for t in range(3):
            w = stage[s, :, t].reshape(STAGE_ROWS, HEADS * HEAD_DIM)
            for half in range(2):
                p = k * 6 + 2 * t + half
                ring[p // 4][p % 4, r, :] = w[:, half * PN:(half + 1) * PN]

    def relayout_chunk(k):
        def step(off, carry):
            stage_copy(k * 4 + off).wait()
            relayout(k, off)
            if k < NK - 1:
                stage_copy(k * 4 + off + STAGES).start()
            return carry

        lax.fori_loop(0, 4, step, 0)

    for k in range(3):
        relayout_chunk(k)
    pltpu.make_async_copy(vec_f32.at[pl.ds(0, 2)], vec_f32.at[pl.ds(2, 2)], small_sem.at[1]).wait()
    pltpu.make_async_copy(vec_bf, vec_bf, small_sem.at[2]).wait()
    bqkv_copy.wait()
    for i in (G2, B2):
        f32_row(i)
    for i in range(3):
        vals = vec_bf[i].astype(F32)
        for j in range(32):
            rows[4 + i, :, j * 128:(j + 1) * 128] = vals[j:j + 1, :]
    for t in range(3):
        vals = bqkv_v[t].astype(F32)
        for j in range(HEADS):
            bqkv_row[:, (t * HEADS + j) * 128:(t * HEADS + j + 1) * 128] = vals[j:j + 1, :]

    def token_place(axis):
        t = lax.broadcasted_iota(jnp.int32, (TOKENS, TOKENS), axis)
        d = sum((t >= ROWS * i).astype(jnp.int32) for i in range(1, 4))
        t = t - ROWS * d
        b = sum((t >= BLOCK * i).astype(jnp.int32) for i in range(1, N_BATCH))
        return b, d * BLOCK + t - BLOCK * b

    (q_seq, q_pos), (k_seq, k_pos) = token_place(0), token_place(1)
    square[...] = jnp.zeros_like(square)
    mask[...] = ((q_seq == k_seq) & (q_pos >= k_pos)).astype(F32)
    ag1_forward(0)
    ag1_forward(1)
    relayout_chunk(3)
    for g in range(G_OUT, RING):
        load_group(g)
    def all_rows(ref, start, size):
        return ref[:, :, start:start + size].reshape(TOKENS, size)

    def qkv_block(chunks):
        for c in chunks:
            ag1(FAR, far, partner, c).wait_recv()
        first, last = chunks[0] == 0, chunks[-1] == NK - 1
        for n in range(6):
            part = None if first else all_rows(acc, n * PN, PN)
            for c in chunks:
                p = c * 6 + n
                term = jnp.dot(all_rows(h_all, *AG1_CHUNKS[c]), ring[p // 4][p % 4], preferred_element_type=F32)
                part = term if part is None else part + term
            if last:
                qkv_bf[:, n * PN:(n + 1) * PN] = (part + bqkv_row[:, n * PN:(n + 1) * PN]).astype(BF16)
            else:
                acc[:, :, n * PN:(n + 1) * PN] = part.reshape(4, ROWS, PN)
        for g in range(chunks[0] * 6 // 4, (chunks[-1] + 1) * 6 // 4):
            load_group(g + RING)

    ag1_partner(partner).wait_recv()
    ag1_forward(2)
    qkv_block((0,))
    ag1_forward(3)
    qkv_block((1,))
    qkv_block((2, 3))

    keep = mask[...] > 0.5
    for first in range(0, HEADS, 4):
        heads = range(first, first + 4)

        def part_of(t, j):
            return qkv_bf[:, (t * HEADS + j) * HEAD_DIM:(t * HEADS + j + 1) * HEAD_DIM]

        logits = [lax.dot_general(part_of(0, j), part_of(1, j), (((1,), (1,)), ((), ())), preferred_element_type=F32) for j in heads]
        logits = [jnp.where(keep, x * HEAD_DIM ** -0.5, -1e30) for x in logits]
        tops = [jnp.max(x, axis=-1, keepdims=True) for x in logits]
        es = [jnp.exp(x - t) for x, t in zip(logits, tops)]
        sums = [jnp.sum(e, axis=-1, keepdims=True) for e in es]
        ps = [(e * (1.0 / z)).astype(BF16) for e, z in zip(es, sums)]
        for j, p in zip(heads, ps):
            ctx[:, j * HEAD_DIM:(j + 1) * HEAD_DIM] = jnp.dot(p, part_of(2, j), preferred_element_type=F32).astype(BF16)

    def reduction(psend, prec, xsend, xrec, send):
        def pair(n):
            at = (slice(None), slice(None), pl.ds(*RS_CHUNKS[n]))
            return remote(psend.at[at], prec.at[at], send_sem.at[send], rs_sem.at[0, n], partner)

        def across(n):
            at = (slice(None), pl.ds(*RS_CHUNKS[n]))
            return remote(xsend.at[at], xrec.at[at], send_sem.at[send + 1], rs_sem.at[1, n], cross)

        def to_pair(n, part):
            cols = pl.ds(*RS_CHUNKS[n])
            acc[:, :, cols] = part.reshape(4, ROWS, RS_CHUNKS[n][1])
            for q in range(2):
                psend[q, :, cols] = acc[2 * q + other_core, :, cols].astype(BF16)
            pair(n).start()

        def to_cross(n):
            cols = pl.ds(*RS_CHUNKS[n])
            pair(n).wait_recv()
            xsend[:, cols] = (acc[2 * other_chip + core, :, cols] + prec[other_chip, :, cols].astype(F32)).astype(BF16)
            across(n).start()

        def total(n):
            cols = pl.ds(*RS_CHUNKS[n])
            across(n).wait_recv()
            return acc[me, :, cols] + prec[chip, :, cols].astype(F32) + xrec[:, cols].astype(F32)

        def drain():
            remote(psend, prec, send_sem.at[send], rs_sem.at[0, 0], partner).wait_send()
            remote(xsend, xrec, send_sem.at[send + 1], rs_sem.at[1, 0], cross).wait_send()

        return to_pair, to_cross, total, drain

    NR = len(RS_CHUNKS)
    rs1_pair, rs1_cross, rs1_total, rs1_drain = reduction(psend1, prec1, xsend1, xrec1, SEND_RS1)
    rs2_pair, rs2_cross, rs2_total, rs2_drain = reduction(psend2, prec2, xsend2, xrec2, SEND_RS2)

    def ag2(which, block, peer, c):
        return push(x1_all, AG2_CHUNKS, SEND_AG2, which, block, peer, c)

    def st(block, peer):
        return remote(stats.at[block], stats.at[block], send_sem.at[SEND_ST], st_sem.at[0], peer)

    ctx_rows = ctx[...]
    lead = 2
    for g in range(G_OUT, G_UP):
        await_group(g)
    for n, (start, size) in enumerate(RS_CHUNKS):
        g, m = G_OUT + start // PN // 4, start // PN % 4
        rs1_pair(n, jnp.dot(ctx_rows, ring[g % RING][m, :, start % PN:start % PN + size], preferred_element_type=F32))
        if n >= lead:
            rs1_cross(n - lead)
    for g in range(G_OUT, G_UP):
        load_group(g + RING)
    for n in range(NR - lead, NR):
        rs1_cross(n)
    for n, (start, size) in enumerate(RS_CHUNKS):
        cols = pl.ds(start, size)
        x1 = (x_own[:, cols].astype(F32) + (rs1_total(n) + rows[BOUT, :, cols])).astype(BF16)
        x1_all[me, :, cols] = x1
        x1 = x1.astype(F32)
        part_mean = jnp.mean(x1, axis=-1, keepdims=True)
        part_dist = jnp.sum((x1 - part_mean) * (x1 - part_mean), axis=-1, keepdims=True)
        if n == 0:
            mean, dist = part_mean, part_dist
        else:
            step = part_mean - mean
            mean = mean + step * (size / (start + size))
            dist = dist + part_dist + step * step * (start * size / (start + size))
        if start + size == sum(AG2_CHUNKS[0]):
            ag2(CROSS, me, cross, 0).start()
            ag2(PARTNER, me, partner, 0).start()
    lane = lax.broadcasted_iota(jnp.int32, (ROWS, 128), 1)
    square[0:ROWS, :] = jnp.where(lane == 0, mean, lax.rsqrt(dist * (1.0 / D) + LN_EPS))
    stats[me] = square[...].T[:8]
    for peer in (cross, far, partner):
        st(me, peer).start()
    for c in range(1, len(AG2_CHUNKS)):
        ag2(CROSS, me, cross, c).start()
        ag2(PARTNER, me, partner, c).start()

    def ag2_forward(c):
        ag2(CROSS, cross, cross, c).wait_recv()
        ag2(FAR, cross, partner, c).start()

    def normalize(c, blocks):
        start, size = AG2_CHUNKS[c]
        cols = pl.ds(start, size)
        to = (h2_even, h2_odd)[c % 2]
        for d in blocks:
            xf = x1_all[d, :, cols].astype(F32)
            to[d, :, 0:size] = ((xf - stat_cols[d, :, 0:1]) * stat_cols[d, :, 1:2] * rows[G2, :, cols] + rows[B2, :, cols]).astype(BF16)

    def gelu(x):
        scale = (2 / math.pi) ** 0.5
        halved = 0.5 * x
        return halved + halved * jnp.tanh(x * (scale + (scale * 0.044715) * (x * x)))

    def blocks_of(c):
        start, size = AG2_CHUNKS[c]
        edges = sorted({start, start + size} | {k * PK for k in range(NK) if start < k * PK < start + size})
        return [(lo // PK, lo % PK, hi - lo) for lo, hi in zip(edges, edges[1:])]

    def up_half(c, half):
        h = all_rows((h2_even, h2_odd)[c % 2], 0, AG2_CHUNKS[c][1])
        for n in range(half * 4, half * 4 + 4):
            part, done = all_rows(acc, n * PN, PN) if c else rows[BUP, :, n * PN:(n + 1) * PN], 0
            total = None
            for k, row, size in blocks_of(c):
                term = jnp.dot(h[:, done:done + size], ring[(G_UP + k * 2 + half) % RING][n % 4, row:row + size, :], preferred_element_type=F32)
                total, done = term if total is None else total + term, done + size
            part = total + part
            if c < len(AG2_CHUNKS) - 1:
                acc[:, :, n * PN:(n + 1) * PN] = part.reshape(4, ROWS, PN)
            else:
                u[:, n * PN:(n + 1) * PN] = gelu(part).astype(BF16)

    def down_sum(n):
        total = None
        for k in range(NK):
            term = jnp.dot(u[:, k * PK:(k + 1) * PK], ring[(G_DOWN + n) % RING][k], preferred_element_type=F32)
            total = term if total is None else total + term
        return total

    ag2_forward(0)
    remote(stats.at[pl.ds(0, 3)], stats.at[pl.ds(0, 3)], send_sem.at[SEND_ST], st_sem.at[0], partner).wait_recv()
    for d in range(4):
        square[0:8, :] = stats[d]
        stat_cols[d] = square[...].T[:ROWS]
    ag2(PARTNER, partner, partner, 0).wait_recv()
    ag2(FAR, far, partner, 0).wait_recv()
    normalize(0, range(4))
    for c in range(len(AG2_CHUNKS) - 1):
        for k, row, size in blocks_of(c):
            if row == 0:
                await_group(G_UP + 2 * k)
                await_group(G_UP + 2 * k + 1)
        up_half(c, 0)
        ag2_forward(c + 1)
        ag2(PARTNER, partner, partner, c + 1).wait_recv()
        normalize(c + 1, (me, partner, cross))
        up_half(c, 1)
        for k, row, size in blocks_of(c):
            if row + size == PK:
                load_group(G_UP + 2 * k + RING)
                load_group(G_UP + 2 * k + 1 + RING)
        ag2(FAR, far, partner, c + 1).wait_recv()
        normalize(c + 1, (far,))

    await_group(G_DOWN)
    for half in range(2):
        up_half(len(AG2_CHUNKS) - 1, half)
    rs2_pair(0, down_sum(0))
    load_group(G_DOWN - 2 + RING)
    load_group(G_DOWN - 1 + RING)
    for n in range(1, NR):
        await_group(G_DOWN + n)
        rs2_pair(n, down_sum(n))
        rs2_cross(n - 1)
    rs2_cross(NR - 1)
    for n, (start, size) in enumerate(RS_CHUNKS):
        cols = pl.ds(start, size)
        out_ref[:, cols] = (x1_all[me, :, cols].astype(F32) + (rs2_total(n) + rows[BDOWN, :, cols])).astype(BF16)

    for buf, send in ((h_all, SEND_AG1), (x1_all, SEND_AG2), (stats, SEND_ST)):
        remote(buf.at[pl.ds(0, 3)], buf.at[pl.ds(0, 3)], send_sem.at[send], st_sem.at[0], partner).wait_send()
    rs1_drain()
    rs2_drain()


def solution(mesh):
    def device_body(hidden, ln1_gain, ln1_bias, w_qkv, b_qkv, w_out, b_out, ln2_gain, ln2_bias, w_up, b_up, w_down, b_down):
        args = (hidden.reshape(ROWS, D), ln1_gain.reshape(32, 128), ln1_bias.reshape(32, 128), w_qkv, b_qkv, w_out.reshape(HEADS * HEAD_DIM, D),
                b_out.reshape(32, 128), ln2_gain.reshape(32, 128), ln2_bias.reshape(32, 128), w_up, b_up.reshape(32, 128), w_down.reshape(NK, PK, D), b_down.reshape(32, 128))
        hbm = pl.BlockSpec(memory_space=pltpu.HBM)
        dma = pltpu.SemaphoreType.DMA
        rs_buffers = [pltpu.VMEM((2, ROWS, D), BF16), pltpu.VMEM((2, ROWS, D), BF16), pltpu.VMEM((ROWS, D), BF16), pltpu.VMEM((ROWS, D), BF16)]
        result = pl.pallas_call(
            kernel,
            out_shape=pltpu.VMEM((ROWS, D), BF16),
            in_specs=[hbm] * len(args),
            out_specs=pl.BlockSpec(memory_space=pltpu.VMEM),
            scratch_shapes=[
                pltpu.VMEM((STAGES, STAGE_ROWS, 3, HEADS, HEAD_DIM), BF16),
                pltpu.VMEM((ROWS, D), BF16),
                pltpu.VMEM((4, ROWS, D), BF16),
                pltpu.VMEM((4, ROWS, D), BF16),
                pltpu.VMEM((4, ROWS, PK), BF16),
                pltpu.VMEM((4, ROWS, PK), BF16),
                pltpu.VMEM((4, ROWS, FF), F32),
                pltpu.VMEM((TOKENS, QKV), BF16),
                pltpu.VMEM((TOKENS, HEADS * HEAD_DIM), BF16),
                pltpu.VMEM((TOKENS, FF), BF16),
                *rs_buffers,
                *rs_buffers,
                pltpu.VMEM((4, 8, 128), F32),
                pltpu.VMEM((4, ROWS, 128), F32),
                pltpu.VMEM((128, 128), F32),
                pltpu.VMEM((4, 32, 128), F32),
                pltpu.VMEM((3, 32, 128), BF16),
                pltpu.VMEM((3, HEADS, HEAD_DIM), BF16),
                pltpu.VMEM((7, 1, D), F32),
                pltpu.VMEM((1, QKV), F32),
                pltpu.VMEM((TOKENS, TOKENS), F32),
                dma((STAGES,)), dma((RING,)), dma((5,)), dma((7,)), dma((3, len(AG2_CHUNKS))), dma((1,)), dma((2, len(RS_CHUNKS))),
                *[pltpu.VMEM((4, PK, PN), BF16)] * RING,
            ],
            compiler_params=pltpu.CompilerParams(collective_id=0, has_side_effects=True, vmem_limit_bytes=62 * 2**20),
            name="decoder_layer",
        )(*args)
        return result.reshape(hidden.shape)

    in_layout = (P("dp", "tp", None), P(), P(), P(None, None, "tp", None), P(None, "tp", None), P("tp", None, None), P(), P(), P(), P(None, "tp"), P("tp"), P("tp", None), P())
    return jax.shard_map(device_body, mesh=mesh, in_specs=in_layout, out_specs=P("dp", "tp", None), check_vma=False)
```

```python
import math

import jax
import jax.numpy as jnp
from jax import lax
from jax.experimental import pallas as pl
from jax.experimental.pallas import tpu as pltpu
from jax.sharding import PartitionSpec as P

MESH = pl.DeviceIdType.MESH
F32, BF16 = jnp.float32, jnp.bfloat16

LN_EPS = 1e-5
N_BATCH, BLOCK, D = 3, 16, 4096
ROWS = N_BATCH * BLOCK
TOKENS = 4 * ROWS
HEADS, HEAD_DIM = 8, 128
FF = 4096
QKV = 3 * HEADS * HEAD_DIM

PK, PN = 1024, 512
DIRECT = 256
NK, NN = D // PK, D // PN
AG1_CHUNKS = [(k * PK, PK) for k in range(NK)]
AG2_CHUNKS = [(0, 1024), (1024, 512), (1536, 1024), (2560, 1024), (3584, 512)]
RS1_CHUNKS = [(DIRECT, PN - DIRECT)] + [(n * PN, PN) for n in range(1, NN)]
RS2_CHUNKS = [(n * PN, PN) for n in range(NN)]
RING = 9
G_OUT, G_UP, G_DOWN, G_END = 6, 8, 16, 24
STAGE_ROWS, STAGES = 256, 4
STEPS = D // STAGE_ROWS


def kernel(x_hbm, g1_hbm, b1_hbm, wqkv_hbm, bqkv_hbm, wout_hbm, bout_hbm, g2_hbm, b2_hbm, wup_hbm, bup_hbm, wdown_hbm, bdown_hbm, out_ref,
           stage, x_own, h_all, x1_all, h2_even, h2_odd, acc, qkv_bf, ctx, u,
           dsend, drec, psend1, prec1, xsend1, xrec1, psend2, prec2, xsend2, xrec2, stats, stat_cols, square,
           vec_f32, vec_bf, bqkv_v, rows, bqkv_row, mask,
           stage_sem, ring_sem, small_sem, send_sem, gather_sem, st_sem, rs_sem, *ring):
    dp = lax.axis_index("dp")
    me = lax.axis_index("tp")
    core = lax.rem(me, 2)
    chip = lax.div(me, 2)
    partner = me + 1 - 2 * core
    cross = lax.rem(me + 2, 4)
    far = lax.rem(partner + 2, 4)
    other_core = 1 - core
    other_chip = 1 - chip
    SEND_AG1, SEND_AG2, SEND_ST, SEND_RS1, SEND_RS2, SEND_DIRECT = 0, 1, 2, 3, 5, 7

    def remote(src, dst, send, recv, peer):
        return pltpu.make_async_remote_copy(src_ref=src, dst_ref=dst, send_sem=send, recv_sem=recv, device_id=(dp, peer), device_id_type=MESH)

    def stage_copy(i):
        return pltpu.make_async_copy(wqkv_hbm.at[pl.ds(i * STAGE_ROWS, STAGE_ROWS)], stage.at[lax.rem(i, STAGES)], stage_sem.at[lax.rem(i, STAGES)])

    def load_group(g):
        to, sem = ring[g % RING], ring_sem.at[g % RING]
        if g >= G_END:
            return
        if g >= G_DOWN:
            pltpu.make_async_copy(wdown_hbm.at[:, :, pl.ds((g - G_DOWN) * PN, PN)], to, sem).start()
            return
        for m in range(4):
            if g >= G_UP:
                k, n = (g - G_UP) // 2, (g - G_UP) % 2 * 4 + m
                src = wup_hbm.at[pl.ds(k * PK, PK), pl.ds(n * PN, PN)]
            else:
                src = wout_hbm.at[:, pl.ds(((g - G_OUT) * 4 + m) * PN, PN)]
            pltpu.make_async_copy(src, to.at[m], sem).start()

    def await_group(g):
        pltpu.make_async_copy(wdown_hbm.at[:, :, pl.ds(0, PN)], ring[g % RING], ring_sem.at[g % RING]).wait()

    barrier = pltpu.get_barrier_semaphore()
    for peer in (partner, cross, far):
        pl.semaphore_signal(barrier, inc=1, device_id=(dp, peer), device_id_type=MESH)
    G1, B1, G2, B2, BOUT, BUP, BDOWN = range(7)
    x_copy = pltpu.make_async_copy(x_hbm, x_own, small_sem.at[4])
    for i, src in enumerate((g1_hbm, b1_hbm)):
        pltpu.make_async_copy(src, vec_f32.at[i], small_sem.at[0]).start()
    x_copy.start()
    stage_copy(0).start()

    def f32_row(i):
        for j in range(32):
            rows[i, :, j * 128:(j + 1) * 128] = vec_f32[i, j:j + 1, :]

    def row_stats(x):
        mean = jnp.mean(x, axis=-1, keepdims=True)
        centered = x - mean
        var = jnp.mean(centered * centered, axis=-1, keepdims=True)
        return mean, lax.rsqrt(var + LN_EPS)

    pltpu.make_async_copy(vec_f32.at[pl.ds(2, 2)], vec_f32.at[pl.ds(0, 2)], small_sem.at[0]).wait()
    for i in (G1, B1):
        f32_row(i)
    stage_copy(1).start()
    x_copy.wait()
    for i in range(2, STAGES):
        stage_copy(i).start()
    for i, src in enumerate((g2_hbm, b2_hbm)):
        pltpu.make_async_copy(src, vec_f32.at[2 + i], small_sem.at[1]).start()
    for i, src in enumerate((bout_hbm, bup_hbm, bdown_hbm)):
        pltpu.make_async_copy(src, vec_bf.at[i], small_sem.at[2]).start()
    bqkv_copy = pltpu.make_async_copy(bqkv_hbm, bqkv_v, small_sem.at[3])
    bqkv_copy.start()
    for b in range(N_BATCH):
        r = pl.ds(b * BLOCK, BLOCK)
        xf = x_own[r, :].astype(F32)
        mean, rstd = row_stats(xf)
        h_all[me, r, :] = ((xf - mean) * rstd * rows[G1] + rows[B1]).astype(BF16)

    pl.semaphore_wait(barrier, 3)

    PARTNER, CROSS, FAR = range(3)

    def push(buf, chunks, send, which, block, peer, c):
        ref = buf.at[block, :, pl.ds(*chunks[c])]
        return remote(ref, ref, send_sem.at[send], gather_sem.at[which, c], peer)

    def ag1(which, block, peer, c):
        return push(h_all, AG1_CHUNKS, SEND_AG1, which, block, peer, c)

    def ag1_partner(block):
        return remote(h_all.at[block], h_all.at[block], send_sem.at[SEND_AG1], gather_sem.at[PARTNER, 0], partner)

    for c in range(NK):
        ag1(CROSS, me, cross, c).start()
    ag1_partner(me).start()

    def ag1_forward(c):
        ag1(CROSS, cross, cross, c).wait_recv()
        ag1(FAR, cross, partner, c).start()

    def relayout(k, off):
        s = lax.rem(k * 4 + off, STAGES)
        r = pl.ds(pl.multiple_of(off * STAGE_ROWS, STAGE_ROWS), STAGE_ROWS)
        for t in range(3):
            w = stage[s, :, t].reshape(STAGE_ROWS, HEADS * HEAD_DIM)
            for half in range(2):
                p = k * 6 + 2 * t + half
                ring[p // 4][p % 4, r, :] = w[:, half * PN:(half + 1) * PN]

    def relayout_chunk(k):
        def step(off, carry):
            stage_copy(k * 4 + off).wait()
            relayout(k, off)
            if k < NK - 1:
                stage_copy(k * 4 + off + STAGES).start()
            return carry

        lax.fori_loop(0, 4, step, 0)

    for k in range(3):
        relayout_chunk(k)
    pltpu.make_async_copy(vec_f32.at[pl.ds(0, 2)], vec_f32.at[pl.ds(2, 2)], small_sem.at[1]).wait()
    pltpu.make_async_copy(vec_bf, vec_bf, small_sem.at[2]).wait()
    bqkv_copy.wait()
    for i in (G2, B2):
        f32_row(i)
    for i in range(3):
        vals = vec_bf[i].astype(F32)
        for j in range(32):
            rows[4 + i, :, j * 128:(j + 1) * 128] = vals[j:j + 1, :]
    for t in range(3):
        vals = bqkv_v[t].astype(F32)
        for j in range(HEADS):
            bqkv_row[:, (t * HEADS + j) * 128:(t * HEADS + j + 1) * 128] = vals[j:j + 1, :]

    def token_place(axis):
        t = lax.broadcasted_iota(jnp.int32, (TOKENS, TOKENS), axis)
        d = sum((t >= ROWS * i).astype(jnp.int32) for i in range(1, 4))
        t = t - ROWS * d
        b = sum((t >= BLOCK * i).astype(jnp.int32) for i in range(1, N_BATCH))
        return b, d * BLOCK + t - BLOCK * b

    (q_seq, q_pos), (k_seq, k_pos) = token_place(0), token_place(1)
    square[...] = jnp.zeros_like(square)
    mask[...] = ((q_seq == k_seq) & (q_pos >= k_pos)).astype(F32)
    ag1_forward(0)
    ag1_forward(1)
    relayout_chunk(3)
    for g in range(G_OUT, RING):
        load_group(g)
    def all_rows(ref, start, size):
        return ref[:, :, start:start + size].reshape(TOKENS, size)

    def qkv_block(chunks):
        for c in chunks:
            ag1(FAR, far, partner, c).wait_recv()
        first, last = chunks[0] == 0, chunks[-1] == NK - 1
        for n in range(6):
            part = None if first else all_rows(acc, n * PN, PN)
            for c in chunks:
                p = c * 6 + n
                term = jnp.dot(all_rows(h_all, *AG1_CHUNKS[c]), ring[p // 4][p % 4], preferred_element_type=F32)
                part = term if part is None else part + term
            if last:
                qkv_bf[:, n * PN:(n + 1) * PN] = (part + bqkv_row[:, n * PN:(n + 1) * PN]).astype(BF16)
            else:
                acc[:, :, n * PN:(n + 1) * PN] = part.reshape(4, ROWS, PN)
        for g in range(chunks[0] * 6 // 4, (chunks[-1] + 1) * 6 // 4):
            load_group(g + RING)

    ag1_partner(partner).wait_recv()
    ag1_forward(2)
    qkv_block((0,))
    ag1_forward(3)
    qkv_block((1,))
    qkv_block((2, 3))

    keep = mask[...] > 0.5
    for first in range(0, HEADS, 4):
        heads = range(first, first + 4)

        def part_of(t, j):
            return qkv_bf[:, (t * HEADS + j) * HEAD_DIM:(t * HEADS + j + 1) * HEAD_DIM]

        logits = [lax.dot_general(part_of(0, j), part_of(1, j), (((1,), (1,)), ((), ())), preferred_element_type=F32) for j in heads]
        logits = [jnp.where(keep, x * HEAD_DIM ** -0.5, -1e30) for x in logits]
        tops = [jnp.max(x, axis=-1, keepdims=True) for x in logits]
        es = [jnp.exp(x - t) for x, t in zip(logits, tops)]
        sums = [jnp.sum(e, axis=-1, keepdims=True) for e in es]
        ps = [(e * (1.0 / z)).astype(BF16) for e, z in zip(es, sums)]
        for j, p in zip(heads, ps):
            ctx[:, j * HEAD_DIM:(j + 1) * HEAD_DIM] = jnp.dot(p, part_of(2, j), preferred_element_type=F32).astype(BF16)

    def reduction(chunks, psend, prec, xsend, xrec, send):
        def pair(n):
            at = (slice(None), slice(None), pl.ds(*chunks[n]))
            return remote(psend.at[at], prec.at[at], send_sem.at[send], rs_sem.at[0, n], partner)

        def across(n):
            at = (slice(None), pl.ds(*chunks[n]))
            return remote(xsend.at[at], xrec.at[at], send_sem.at[send + 1], rs_sem.at[1, n], cross)

        def to_pair(n):
            cols = pl.ds(*chunks[n])
            for q in range(2):
                psend[q, :, cols] = acc[2 * q + other_core, :, cols].astype(BF16)
            pair(n).start()

        def to_cross(n):
            cols = pl.ds(*chunks[n])
            pair(n).wait_recv()
            xsend[:, cols] = (acc[2 * other_chip + core, :, cols] + prec[other_chip, :, cols].astype(F32)).astype(BF16)
            across(n).start()

        def total(n):
            cols = pl.ds(*chunks[n])
            across(n).wait_recv()
            return acc[me, :, cols] + prec[chip, :, cols].astype(F32) + xrec[:, cols].astype(F32)

        def drain():
            rest = pl.ds(chunks[0][0], D - chunks[0][0])
            at, sems = (slice(None), slice(None), rest), (send_sem.at[send], rs_sem.at[0, 0])
            remote(psend.at[at], prec.at[at], *sems, partner).wait_send()
            at, sems = (slice(None), rest), (send_sem.at[send + 1], rs_sem.at[1, 0])
            remote(xsend.at[at], xrec.at[at], *sems, cross).wait_send()

        return to_pair, to_cross, total, drain

    NR = len(RS1_CHUNKS)
    rs1_pair, rs1_cross, rs1_total, rs1_drain = reduction(RS1_CHUNKS, psend1, prec1, xsend1, xrec1, SEND_RS1)
    rs2_pair, rs2_cross, rs2_total, rs2_drain = reduction(RS2_CHUNKS, psend2, prec2, xsend2, xrec2, SEND_RS2)

    def ag2(which, block, peer, c):
        return push(x1_all, AG2_CHUNKS, SEND_AG2, which, block, peer, c)

    def st(block, peer):
        return remote(stats.at[block], stats.at[block], send_sem.at[SEND_ST], st_sem.at[0], peer)

    def direct(i):
        return remote(dsend.at[i], drec.at[i], send_sem.at[SEND_DIRECT], rs_sem.at[0, NR], (cross, far, partner)[i])

    def direct_total():
        remote(dsend, drec, send_sem.at[SEND_DIRECT], rs_sem.at[0, NR], cross).wait_recv()
        total = acc[me, :, 0:DIRECT]
        for i in (2, 0, 1):
            total = total + drec[i].astype(F32)
        return total

    ctx_rows = ctx[...]
    lead = 2
    for g in range(G_OUT, G_UP):
        await_group(g)
    for n in range(NR):
        part = jnp.dot(ctx_rows, ring[(G_OUT + n // 4) % RING][n % 4], preferred_element_type=F32)
        acc[:, :, n * PN:(n + 1) * PN] = part.reshape(4, ROWS, PN)
        if n == 0:
            for i, peer in enumerate((cross, far, partner)):
                dsend[i] = acc[peer, :, 0:DIRECT].astype(BF16)
            for i in range(3):
                direct(i).start()
        rs1_pair(n)
        if n >= lead:
            rs1_cross(n - lead)
    for g in range(G_OUT, G_UP):
        load_group(g + RING)
    for n in range(NR - lead, NR):
        rs1_cross(n)
    for n, (start, size) in enumerate([(0, DIRECT)] + RS1_CHUNKS):
        cols = pl.ds(start, size)
        total = rs1_total(n - 1) if n else direct_total()
        x1 = (x_own[:, cols].astype(F32) + (total + rows[BOUT, :, cols])).astype(BF16)
        x1_all[me, :, cols] = x1
        x1 = x1.astype(F32)
        part_mean = jnp.mean(x1, axis=-1, keepdims=True)
        part_dist = jnp.sum((x1 - part_mean) * (x1 - part_mean), axis=-1, keepdims=True)
        if n == 0:
            mean, dist = part_mean, part_dist
        else:
            step = part_mean - mean
            mean = mean + step * (size / (start + size))
            dist = dist + part_dist + step * step * (start * size / (start + size))
        if start + size == sum(AG2_CHUNKS[0]):
            ag2(CROSS, me, cross, 0).start()
            ag2(PARTNER, me, partner, 0).start()
    lane = lax.broadcasted_iota(jnp.int32, (ROWS, 128), 1)
    square[0:ROWS, :] = jnp.where(lane == 0, mean, lax.rsqrt(dist * (1.0 / D) + LN_EPS))
    stats[me] = square[...].T[:8]
    for peer in (cross, far, partner):
        st(me, peer).start()
    for c in range(1, len(AG2_CHUNKS)):
        ag2(CROSS, me, cross, c).start()
        ag2(PARTNER, me, partner, c).start()

    def ag2_forward(c):
        ag2(CROSS, cross, cross, c).wait_recv()
        ag2(FAR, cross, partner, c).start()

    def normalize(c, blocks):
        start, size = AG2_CHUNKS[c]
        cols = pl.ds(start, size)
        to = (h2_even, h2_odd)[c % 2]
        for d in blocks:
            xf = x1_all[d, :, cols].astype(F32)
            to[d, :, 0:size] = ((xf - stat_cols[d, :, 0:1]) * stat_cols[d, :, 1:2] * rows[G2, :, cols] + rows[B2, :, cols]).astype(BF16)

    def gelu(x):
        scale = (2 / math.pi) ** 0.5
        halved = 0.5 * x
        return halved + halved * jnp.tanh(x * (scale + (scale * 0.044715) * (x * x)))

    def blocks_of(c):
        start, size = AG2_CHUNKS[c]
        edges = sorted({start, start + size} | {k * PK for k in range(NK) if start < k * PK < start + size})
        return [(lo // PK, lo % PK, hi - lo) for lo, hi in zip(edges, edges[1:])]

    def up_panels(c, panels):
        h = all_rows((h2_even, h2_odd)[c % 2], 0, AG2_CHUNKS[c][1])
        for n in panels:
            part, done = all_rows(acc, n * PN, PN) if c else rows[BUP, :, n * PN:(n + 1) * PN], 0
            total = None
            for k, row, size in blocks_of(c):
                term = jnp.dot(h[:, done:done + size], ring[(G_UP + k * 2 + n // 4) % RING][n % 4, row:row + size, :], preferred_element_type=F32)
                total, done = term if total is None else total + term, done + size
            part = total + part
            if c < len(AG2_CHUNKS) - 1:
                acc[:, :, n * PN:(n + 1) * PN] = part.reshape(4, ROWS, PN)
            else:
                u[:, n * PN:(n + 1) * PN] = gelu(part).astype(BF16)

    def down_sum(n):
        total = None
        for k in range(NK):
            term = jnp.dot(u[:, k * PK:(k + 1) * PK], ring[(G_DOWN + n) % RING][k], preferred_element_type=F32)
            total = term if total is None else total + term
        return total

    def down_to_pair(n):
        acc[:, :, n * PN:(n + 1) * PN] = down_sum(n).reshape(4, ROWS, PN)
        rs2_pair(n)

    ag2_forward(0)
    remote(stats.at[pl.ds(0, 3)], stats.at[pl.ds(0, 3)], send_sem.at[SEND_ST], st_sem.at[0], partner).wait_recv()
    for d in range(4):
        square[0:8, :] = stats[d]
        stat_cols[d] = square[...].T[:ROWS]
    ag2(PARTNER, partner, partner, 0).wait_recv()
    ag2(FAR, far, partner, 0).wait_recv()
    normalize(0, range(4))
    for c in range(len(AG2_CHUNKS) - 1):
        for k, row, size in blocks_of(c):
            if row == 0:
                await_group(G_UP + 2 * k)
                await_group(G_UP + 2 * k + 1)
        before = (3, 5, 4, 0)[c]
        up_panels(c, range(before))
        ag2_forward(c + 1)
        ag2(PARTNER, partner, partner, c + 1).wait_recv()
        normalize(c + 1, (me, partner, cross))
        up_panels(c, range(before, NN))
        for k, row, size in blocks_of(c):
            if row + size == PK:
                load_group(G_UP + 2 * k + RING)
                load_group(G_UP + 2 * k + 1 + RING)
        ag2(FAR, far, partner, c + 1).wait_recv()
        normalize(c + 1, (far,))

    await_group(G_DOWN)
    up_panels(len(AG2_CHUNKS) - 1, range(NN))
    down_to_pair(0)
    load_group(G_DOWN - 2 + RING)
    load_group(G_DOWN - 1 + RING)
    for n in range(1, NR):
        await_group(G_DOWN + n)
        down_to_pair(n)
        rs2_cross(n - 1)
    rs2_cross(NR - 1)
    for n, (start, size) in enumerate(RS2_CHUNKS):
        cols = pl.ds(start, size)
        out_ref[:, cols] = (x1_all[me, :, cols].astype(F32) + (rs2_total(n) + rows[BDOWN, :, cols])).astype(BF16)

    for buf, send in ((h_all, SEND_AG1), (x1_all, SEND_AG2), (stats, SEND_ST)):
        remote(buf.at[pl.ds(0, 3)], buf.at[pl.ds(0, 3)], send_sem.at[send], st_sem.at[0], partner).wait_send()
    rs1_drain()
    remote(dsend, drec, send_sem.at[SEND_DIRECT], rs_sem.at[0, NR], cross).wait_send()
    rs2_drain()


def solution(mesh):
    def device_body(hidden, ln1_gain, ln1_bias, w_qkv, b_qkv, w_out, b_out, ln2_gain, ln2_bias, w_up, b_up, w_down, b_down):
        args = (hidden.reshape(ROWS, D), ln1_gain.reshape(32, 128), ln1_bias.reshape(32, 128), w_qkv, b_qkv, w_out.reshape(HEADS * HEAD_DIM, D),
                b_out.reshape(32, 128), ln2_gain.reshape(32, 128), ln2_bias.reshape(32, 128), w_up, b_up.reshape(32, 128), w_down.reshape(NK, PK, D), b_down.reshape(32, 128))
        hbm = pl.BlockSpec(memory_space=pltpu.HBM)
        dma = pltpu.SemaphoreType.DMA
        rs_buffers = [pltpu.VMEM((2, ROWS, D), BF16), pltpu.VMEM((2, ROWS, D), BF16), pltpu.VMEM((ROWS, D), BF16), pltpu.VMEM((ROWS, D), BF16)]
        result = pl.pallas_call(
            kernel,
            out_shape=pltpu.VMEM((ROWS, D), BF16),
            in_specs=[hbm] * len(args),
            out_specs=pl.BlockSpec(memory_space=pltpu.VMEM),
            scratch_shapes=[
                pltpu.VMEM((STAGES, STAGE_ROWS, 3, HEADS, HEAD_DIM), BF16),
                pltpu.VMEM((ROWS, D), BF16),
                pltpu.VMEM((4, ROWS, D), BF16),
                pltpu.VMEM((4, ROWS, D), BF16),
                pltpu.VMEM((4, ROWS, PK), BF16),
                pltpu.VMEM((4, ROWS, PK), BF16),
                pltpu.VMEM((4, ROWS, FF), F32),
                pltpu.VMEM((TOKENS, QKV), BF16),
                pltpu.VMEM((TOKENS, HEADS * HEAD_DIM), BF16),
                pltpu.VMEM((TOKENS, FF), BF16),
                pltpu.VMEM((3, ROWS, DIRECT), BF16),
                pltpu.VMEM((3, ROWS, DIRECT), BF16),
                *rs_buffers,
                *rs_buffers,
                pltpu.VMEM((4, 8, 128), F32),
                pltpu.VMEM((4, ROWS, 128), F32),
                pltpu.VMEM((128, 128), F32),
                pltpu.VMEM((4, 32, 128), F32),
                pltpu.VMEM((3, 32, 128), BF16),
                pltpu.VMEM((3, HEADS, HEAD_DIM), BF16),
                pltpu.VMEM((7, 1, D), F32),
                pltpu.VMEM((1, QKV), F32),
                pltpu.VMEM((TOKENS, TOKENS), F32),
                dma((STAGES,)), dma((RING,)), dma((5,)), dma((8,)), dma((3, len(AG2_CHUNKS))), dma((1,)), dma((2, NN + 1)),
                *[pltpu.VMEM((4, PK, PN), BF16)] * RING,
            ],
            compiler_params=pltpu.CompilerParams(collective_id=0, has_side_effects=True, vmem_limit_bytes=62 * 2**20),
            name="decoder_layer",
        )(*args)
        return result.reshape(hidden.shape)

    in_layout = (P("dp", "tp", None), P(), P(), P(None, None, "tp", None), P(None, "tp", None), P("tp", None, None), P(), P(), P(), P(None, "tp"), P("tp"), P("tp", None), P())
    return jax.shard_map(device_body, mesh=mesh, in_specs=in_layout, out_specs=P("dp", "tp", None), check_vma=False)
```

```python
import math

import jax
import jax.numpy as jnp
from jax import lax
from jax.experimental import pallas as pl
from jax.experimental.pallas import tpu as pltpu
from jax.sharding import PartitionSpec as P

MESH = pl.DeviceIdType.MESH
F32, BF16 = jnp.float32, jnp.bfloat16

LN_EPS = 1e-5
N_BATCH, BLOCK, D = 3, 16, 4096
ROWS = N_BATCH * BLOCK
TOKENS = 4 * ROWS
HEADS, HEAD_DIM = 8, 128
FF = 4096
QKV = 3 * HEADS * HEAD_DIM

PK, PN = 1024, 512
DIRECT = 256
NK, NN = D // PK, D // PN
AG1_CHUNKS = [(k * PK, PK) for k in range(NK)]
AG2_CHUNKS = [(0, 1024), (1024, 512), (1536, 1024), (2560, 1024), (3584, 512)]
RS1_CHUNKS = [(DIRECT, PN - DIRECT)] + [(n * PN, PN) for n in range(1, NN)]
RS2_CHUNKS = [(n * PN, PN) for n in range(NN)]
RING = 9
G_OUT, G_UP, G_DOWN, G_END = 6, 8, 16, 24
STAGE_ROWS, STAGES = 256, 4
STEPS = D // STAGE_ROWS


def kernel(x_hbm, g1_hbm, b1_hbm, wqkv_hbm, bqkv_hbm, wout_hbm, bout_hbm, g2_hbm, b2_hbm, wup_hbm, bup_hbm, wdown_hbm, bdown_hbm, out_ref,
           stage, x_own, h_all, x1_all, h2_even, h2_odd, acc, qkv_bf, ctx, u,
           dsend, drec, psend1, prec1, xsend1, xrec1, psend2, prec2, xsend2, xrec2, stats, stat_cols, square,
           vec_f32, vec_bf, bqkv_v, rows, bqkv_row, mask,
           stage_sem, ring_sem, small_sem, send_sem, gather_sem, st_sem, rs_sem, *ring):
    dp = lax.axis_index("dp")
    me = lax.axis_index("tp")
    core = lax.rem(me, 2)
    chip = lax.div(me, 2)
    partner = me + 1 - 2 * core
    cross = lax.rem(me + 2, 4)
    far = lax.rem(partner + 2, 4)
    other_core = 1 - core
    other_chip = 1 - chip
    SEND_AG1, SEND_AG2, SEND_ST, SEND_RS1, SEND_RS2, SEND_DIRECT = 0, 1, 2, 3, 5, 7

    def remote(src, dst, send, recv, peer):
        return pltpu.make_async_remote_copy(src_ref=src, dst_ref=dst, send_sem=send, recv_sem=recv, device_id=(dp, peer), device_id_type=MESH)

    def stage_copy(i):
        return pltpu.make_async_copy(wqkv_hbm.at[pl.ds(i * STAGE_ROWS, STAGE_ROWS)], stage.at[lax.rem(i, STAGES)], stage_sem.at[lax.rem(i, STAGES)])

    def load_group(g):
        to, sem = ring[g % RING], ring_sem.at[g % RING]
        if g >= G_END:
            return
        if g >= G_DOWN:
            pltpu.make_async_copy(wdown_hbm.at[:, :, pl.ds((g - G_DOWN) * PN, PN)], to, sem).start()
            return
        for m in range(4):
            if g >= G_UP:
                k, n = (g - G_UP) // 2, (g - G_UP) % 2 * 4 + m
                src = wup_hbm.at[pl.ds(k * PK, PK), pl.ds(n * PN, PN)]
            else:
                src = wout_hbm.at[:, pl.ds(((g - G_OUT) * 4 + m) * PN, PN)]
            pltpu.make_async_copy(src, to.at[m], sem).start()

    def await_group(g):
        pltpu.make_async_copy(wdown_hbm.at[:, :, pl.ds(0, PN)], ring[g % RING], ring_sem.at[g % RING]).wait()

    barrier = pltpu.get_barrier_semaphore()
    for peer in (partner, cross, far):
        pl.semaphore_signal(barrier, inc=1, device_id=(dp, peer), device_id_type=MESH)
    G1, B1, G2, B2, BOUT, BUP, BDOWN = range(7)
    x_copy = pltpu.make_async_copy(x_hbm, x_own, small_sem.at[4])
    for i, src in enumerate((g1_hbm, b1_hbm)):
        pltpu.make_async_copy(src, vec_f32.at[i], small_sem.at[0]).start()
    x_copy.start()
    stage_copy(0).start()

    def f32_row(i):
        for j in range(32):
            rows[i, :, j * 128:(j + 1) * 128] = vec_f32[i, j:j + 1, :]

    def row_stats(x):
        mean = jnp.mean(x, axis=-1, keepdims=True)
        centered = x - mean
        var = jnp.mean(centered * centered, axis=-1, keepdims=True)
        return mean, lax.rsqrt(var + LN_EPS)

    pltpu.make_async_copy(vec_f32.at[pl.ds(2, 2)], vec_f32.at[pl.ds(0, 2)], small_sem.at[0]).wait()
    for i in (G1, B1):
        f32_row(i)
    stage_copy(1).start()
    x_copy.wait()
    for i in range(2, STAGES):
        stage_copy(i).start()
    for i, src in enumerate((g2_hbm, b2_hbm)):
        pltpu.make_async_copy(src, vec_f32.at[2 + i], small_sem.at[1]).start()
    for i, src in enumerate((bout_hbm, bup_hbm, bdown_hbm)):
        pltpu.make_async_copy(src, vec_bf.at[i], small_sem.at[2]).start()
    bqkv_copy = pltpu.make_async_copy(bqkv_hbm, bqkv_v, small_sem.at[3])
    bqkv_copy.start()
    for b in range(N_BATCH):
        r = pl.ds(b * BLOCK, BLOCK)
        xf = x_own[r, :].astype(F32)
        mean, rstd = row_stats(xf)
        h_all[me, r, :] = ((xf - mean) * rstd * rows[G1] + rows[B1]).astype(BF16)

    pl.semaphore_wait(barrier, 3)

    PARTNER, CROSS, FAR = range(3)

    def push(buf, chunks, send, which, block, peer, c):
        ref = buf.at[block, :, pl.ds(*chunks[c])]
        return remote(ref, ref, send_sem.at[send], gather_sem.at[which, c], peer)

    def ag1(which, block, peer, c):
        return push(h_all, AG1_CHUNKS, SEND_AG1, which, block, peer, c)

    def ag1_partner(block):
        return remote(h_all.at[block], h_all.at[block], send_sem.at[SEND_AG1], gather_sem.at[PARTNER, 0], partner)

    for c in range(NK):
        ag1(CROSS, me, cross, c).start()
    ag1_partner(me).start()

    def ag1_forward(c):
        ag1(CROSS, cross, cross, c).wait_recv()
        ag1(FAR, cross, partner, c).start()

    def relayout(k, off):
        s = lax.rem(k * 4 + off, STAGES)
        r = pl.ds(pl.multiple_of(off * STAGE_ROWS, STAGE_ROWS), STAGE_ROWS)
        for t in range(3):
            w = stage[s, :, t].reshape(STAGE_ROWS, HEADS * HEAD_DIM)
            for half in range(2):
                p = k * 6 + 2 * t + half
                ring[p // 4][p % 4, r, :] = w[:, half * PN:(half + 1) * PN]

    def relayout_chunk(k):
        def step(off, carry):
            stage_copy(k * 4 + off).wait()
            relayout(k, off)
            if k < NK - 1:
                stage_copy(k * 4 + off + STAGES).start()
            return carry

        lax.fori_loop(0, 4, step, 0)

    for k in range(3):
        relayout_chunk(k)
    pltpu.make_async_copy(vec_f32.at[pl.ds(0, 2)], vec_f32.at[pl.ds(2, 2)], small_sem.at[1]).wait()
    pltpu.make_async_copy(vec_bf, vec_bf, small_sem.at[2]).wait()
    bqkv_copy.wait()
    for i in (G2, B2):
        f32_row(i)
    for i in range(3):
        vals = vec_bf[i].astype(F32)
        for j in range(32):
            rows[4 + i, :, j * 128:(j + 1) * 128] = vals[j:j + 1, :]
    for t in range(3):
        vals = bqkv_v[t].astype(F32)
        for j in range(HEADS):
            bqkv_row[:, (t * HEADS + j) * 128:(t * HEADS + j + 1) * 128] = vals[j:j + 1, :]

    def token_place(axis):
        t = lax.broadcasted_iota(jnp.int32, (TOKENS, TOKENS), axis)
        d = sum((t >= ROWS * i).astype(jnp.int32) for i in range(1, 4))
        t = t - ROWS * d
        b = sum((t >= BLOCK * i).astype(jnp.int32) for i in range(1, N_BATCH))
        return b, d * BLOCK + t - BLOCK * b

    (q_seq, q_pos), (k_seq, k_pos) = token_place(0), token_place(1)
    square[...] = jnp.zeros_like(square)
    mask[...] = jnp.where(q_seq == k_seq, jnp.where(q_pos >= k_pos, 0.0, -1e30), -jnp.inf).astype(F32)
    ag1_forward(0)
    ag1_forward(1)
    relayout_chunk(3)
    for g in range(G_OUT, RING):
        load_group(g)
    def all_rows(ref, start, size):
        return ref[:, :, start:start + size].reshape(TOKENS, size)

    def part_of(t, j):
        return qkv_bf[:, (t * HEADS + j) * HEAD_DIM:(t * HEADS + j + 1) * HEAD_DIM]

    def scores(heads):
        return [lax.dot_general(part_of(0, j), part_of(1, j), (((1,), (1,)), ((), ())), preferred_element_type=F32) for j in heads]

    def softmax(logits):
        fill = mask[...]
        logits = [jnp.where(fill == 0.0, x * HEAD_DIM ** -0.5, fill) for x in logits]
        tops = [jnp.max(x, axis=-1, keepdims=True) for x in logits]
        es = [jnp.exp(x - t) for x, t in zip(logits, tops)]
        sums = [jnp.sum(e, axis=-1, keepdims=True) for e in es]
        return [(e * (1.0 / z)).astype(BF16) for e, z in zip(es, sums)]

    def weigh(heads, ps):
        for j, p in zip(heads, ps):
            ctx[:, j * HEAD_DIM:(j + 1) * HEAD_DIM] = jnp.dot(p, part_of(2, j), preferred_element_type=F32).astype(BF16)

    def qkv_block(chunks):
        for c in chunks:
            ag1(FAR, far, partner, c).wait_recv()
        first, last = chunks[0] == 0, chunks[-1] == NK - 1
        early = None
        for n in (0, 2, 4, 1, 3, 5):
            part = None if first else all_rows(acc, n * PN, PN)
            for c in chunks:
                p = c * 6 + n
                term = jnp.dot(all_rows(h_all, *AG1_CHUNKS[c]), ring[p // 4][p % 4], preferred_element_type=F32)
                part = term if part is None else part + term
            if last:
                qkv_bf[:, n * PN:(n + 1) * PN] = (part + bqkv_row[:, n * PN:(n + 1) * PN]).astype(BF16)
                if n == 4:
                    early = scores(range(4))
                if n in (1, 3):
                    half = softmax(early[:2])
                    early = early[2:]
                    weigh(range(n - 1, n + 1), half)
            else:
                acc[:, :, n * PN:(n + 1) * PN] = part.reshape(4, ROWS, PN)
        for g in range(chunks[0] * 6 // 4, (chunks[-1] + 1) * 6 // 4):
            load_group(g + RING)

    ag1_partner(partner).wait_recv()
    ag1_forward(2)
    qkv_block((0,))
    ag1_forward(3)
    qkv_block((1,))
    qkv_block((2, 3))

    ps = softmax(scores(range(4, 8)))
    weigh(range(4, 8), ps)

    def reduction(chunks, psend, prec, xsend, xrec, send):
        def pair(n):
            at = (slice(None), slice(None), pl.ds(*chunks[n]))
            return remote(psend.at[at], prec.at[at], send_sem.at[send], rs_sem.at[0, n], partner)

        def across(n):
            at = (slice(None), pl.ds(*chunks[n]))
            return remote(xsend.at[at], xrec.at[at], send_sem.at[send + 1], rs_sem.at[1, n], cross)

        def to_pair(n):
            cols = pl.ds(*chunks[n])
            for q in range(2):
                psend[q, :, cols] = acc[2 * q + other_core, :, cols].astype(BF16)
            pair(n).start()

        def to_cross(n):
            cols = pl.ds(*chunks[n])
            pair(n).wait_recv()
            xsend[:, cols] = (acc[2 * other_chip + core, :, cols] + prec[other_chip, :, cols].astype(F32)).astype(BF16)
            across(n).start()

        def total(n):
            cols = pl.ds(*chunks[n])
            across(n).wait_recv()
            return acc[me, :, cols] + prec[chip, :, cols].astype(F32) + xrec[:, cols].astype(F32)

        def drain():
            rest = pl.ds(chunks[0][0], D - chunks[0][0])
            at, sems = (slice(None), slice(None), rest), (send_sem.at[send], rs_sem.at[0, 0])
            remote(psend.at[at], prec.at[at], *sems, partner).wait_send()
            at, sems = (slice(None), rest), (send_sem.at[send + 1], rs_sem.at[1, 0])
            remote(xsend.at[at], xrec.at[at], *sems, cross).wait_send()

        return to_pair, to_cross, total, drain

    NR = len(RS1_CHUNKS)
    rs1_pair, rs1_cross, rs1_total, rs1_drain = reduction(RS1_CHUNKS, psend1, prec1, xsend1, xrec1, SEND_RS1)
    rs2_pair, rs2_cross, rs2_total, rs2_drain = reduction(RS2_CHUNKS, psend2, prec2, xsend2, xrec2, SEND_RS2)

    def ag2(which, block, peer, c):
        return push(x1_all, AG2_CHUNKS, SEND_AG2, which, block, peer, c)

    def st(block, peer, sem):
        return remote(stats.at[block], stats.at[block], send_sem.at[SEND_ST], st_sem.at[sem], peer)

    def direct(i):
        return remote(dsend.at[i], drec.at[i], send_sem.at[SEND_DIRECT], rs_sem.at[0, NR], (cross, far, partner)[i])

    def direct_total():
        remote(dsend, drec, send_sem.at[SEND_DIRECT], rs_sem.at[0, NR], cross).wait_recv()
        total = acc[me, :, 0:DIRECT]
        for i in (2, 0, 1):
            total = total + drec[i].astype(F32)
        return total

    ctx_rows = ctx[...]
    lead = 2
    for g in range(G_OUT, G_UP):
        await_group(g)
    for n in range(NR):
        part = jnp.dot(ctx_rows, ring[(G_OUT + n // 4) % RING][n % 4], preferred_element_type=F32)
        acc[:, :, n * PN:(n + 1) * PN] = part.reshape(4, ROWS, PN)
        if n == 0:
            for i, peer in enumerate((cross, far, partner)):
                dsend[i] = acc[peer, :, 0:DIRECT].astype(BF16)
            for i in range(3):
                direct(i).start()
        rs1_pair(n)
        if n >= lead:
            rs1_cross(n - lead)
    for g in range(G_OUT, G_UP):
        load_group(g + RING)
    for n in range(NR - lead, NR):
        rs1_cross(n)
    for n, (start, size) in enumerate([(0, DIRECT)] + RS1_CHUNKS):
        cols = pl.ds(start, size)
        total = rs1_total(n - 1) if n else direct_total()
        x1 = (x_own[:, cols].astype(F32) + (total + rows[BOUT, :, cols])).astype(BF16)
        x1_all[me, :, cols] = x1
        x1 = x1.astype(F32)
        part_mean = jnp.mean(x1, axis=-1, keepdims=True)
        part_dist = jnp.sum((x1 - part_mean) * (x1 - part_mean), axis=-1, keepdims=True)
        if n == 0:
            mean, dist = part_mean, part_dist
        else:
            step = part_mean - mean
            mean = mean + step * (size / (start + size))
            dist = dist + part_dist + step * step * (start * size / (start + size))
        if start + size == sum(AG2_CHUNKS[0]):
            ag2(CROSS, me, cross, 0).start()
            ag2(PARTNER, me, partner, 0).start()
    lane = lax.broadcasted_iota(jnp.int32, (ROWS, 128), 1)
    square[0:ROWS, :] = jnp.where(lane == 0, mean, lax.rsqrt(dist * (1.0 / D) + LN_EPS))
    stats[me] = square[...].T[:8]
    for peer in (cross, far):
        st(me, peer, 1).start()
    st(me, partner, 0).start()
    for c in range(1, len(AG2_CHUNKS)):
        ag2(CROSS, me, cross, c).start()
        ag2(PARTNER, me, partner, c).start()

    def ag2_forward(c):
        ag2(CROSS, cross, cross, c).wait_recv()
        ag2(FAR, cross, partner, c).start()

    def normalize(c, blocks):
        start, size = AG2_CHUNKS[c]
        cols = pl.ds(start, size)
        to = (h2_even, h2_odd)[c % 2]
        for d in blocks:
            xf = x1_all[d, :, cols].astype(F32)
            to[d, :, 0:size] = ((xf - stat_cols[d, :, 0:1]) * stat_cols[d, :, 1:2] * rows[G2, :, cols] + rows[B2, :, cols]).astype(BF16)

    def gelu(x):
        scale = (2 / math.pi) ** 0.5
        halved = 0.5 * x
        return halved + halved * jnp.tanh(x * (scale + (scale * 0.044715) * (x * x)))

    def blocks_of(c):
        start, size = AG2_CHUNKS[c]
        edges = sorted({start, start + size} | {k * PK for k in range(NK) if start < k * PK < start + size})
        return [(lo // PK, lo % PK, hi - lo) for lo, hi in zip(edges, edges[1:])]

    def up_panels(c, panels):
        h = all_rows((h2_even, h2_odd)[c % 2], 0, AG2_CHUNKS[c][1])
        for n in panels:
            part, done = all_rows(acc, n * PN, PN) if c else rows[BUP, :, n * PN:(n + 1) * PN], 0
            total = None
            for k, row, size in blocks_of(c):
                term = jnp.dot(h[:, done:done + size], ring[(G_UP + k * 2 + n // 4) % RING][n % 4, row:row + size, :], preferred_element_type=F32)
                total, done = term if total is None else total + term, done + size
            part = total + part
            if c < len(AG2_CHUNKS) - 1:
                acc[:, :, n * PN:(n + 1) * PN] = part.reshape(4, ROWS, PN)
            else:
                u[:, n * PN:(n + 1) * PN] = gelu(part).astype(BF16)

    def down_sum(n):
        total = None
        for k in range(NK):
            term = jnp.dot(u[:, k * PK:(k + 1) * PK], ring[(G_DOWN + n) % RING][k], preferred_element_type=F32)
            total = term if total is None else total + term
        return total

    def down_to_pair(n):
        acc[:, :, n * PN:(n + 1) * PN] = down_sum(n).reshape(4, ROWS, PN)
        rs2_pair(n)

    def columns(d):
        square[0:8, :] = stats[d]
        stat_cols[d] = square[...].T[:ROWS]

    st(partner, partner, 0).wait_recv()
    columns(me)
    columns(partner)
    ag2(PARTNER, partner, partner, 0).wait_recv()
    normalize(0, (me, partner))
    ag2_forward(0)
    remote(stats.at[pl.ds(0, 2)], stats.at[pl.ds(0, 2)], send_sem.at[SEND_ST], st_sem.at[1], cross).wait_recv()
    columns(cross)
    columns(far)
    ag2(FAR, far, partner, 0).wait_recv()
    normalize(0, (cross, far))
    for c in range(len(AG2_CHUNKS) - 1):
        for k, row, size in blocks_of(c):
            if row == 0:
                await_group(G_UP + 2 * k)
                await_group(G_UP + 2 * k + 1)
        before = (3, 5, 4, 0)[c]
        up_panels(c, range(before))
        ag2_forward(c + 1)
        ag2(PARTNER, partner, partner, c + 1).wait_recv()
        normalize(c + 1, (me, partner, cross))
        up_panels(c, range(before, NN))
        for k, row, size in blocks_of(c):
            if row + size == PK:
                load_group(G_UP + 2 * k + RING)
                load_group(G_UP + 2 * k + 1 + RING)
        ag2(FAR, far, partner, c + 1).wait_recv()
        normalize(c + 1, (far,))

    await_group(G_DOWN)
    up_panels(len(AG2_CHUNKS) - 1, range(NN))
    down_to_pair(0)
    load_group(G_DOWN - 2 + RING)
    load_group(G_DOWN - 1 + RING)
    for n in range(1, NR):
        await_group(G_DOWN + n)
        down_to_pair(n)
        rs2_cross(n - 1)
    rs2_cross(NR - 1)
    for n, (start, size) in enumerate(RS2_CHUNKS):
        cols = pl.ds(start, size)
        out_ref[:, cols] = (x1_all[me, :, cols].astype(F32) + (rs2_total(n) + rows[BDOWN, :, cols])).astype(BF16)

    for buf, send in ((h_all, SEND_AG1), (x1_all, SEND_AG2), (stats, SEND_ST)):
        remote(buf.at[pl.ds(0, 3)], buf.at[pl.ds(0, 3)], send_sem.at[send], st_sem.at[0], partner).wait_send()
    rs1_drain()
    remote(dsend, drec, send_sem.at[SEND_DIRECT], rs_sem.at[0, NR], cross).wait_send()
    rs2_drain()


def solution(mesh):
    def device_body(hidden, ln1_gain, ln1_bias, w_qkv, b_qkv, w_out, b_out, ln2_gain, ln2_bias, w_up, b_up, w_down, b_down):
        args = (hidden.reshape(ROWS, D), ln1_gain.reshape(32, 128), ln1_bias.reshape(32, 128), w_qkv, b_qkv, w_out.reshape(HEADS * HEAD_DIM, D),
                b_out.reshape(32, 128), ln2_gain.reshape(32, 128), ln2_bias.reshape(32, 128), w_up, b_up.reshape(32, 128), w_down.reshape(NK, PK, D), b_down.reshape(32, 128))
        hbm = pl.BlockSpec(memory_space=pltpu.HBM)
        dma = pltpu.SemaphoreType.DMA
        rs_buffers = [pltpu.VMEM((2, ROWS, D), BF16), pltpu.VMEM((2, ROWS, D), BF16), pltpu.VMEM((ROWS, D), BF16), pltpu.VMEM((ROWS, D), BF16)]
        result = pl.pallas_call(
            kernel,
            out_shape=pltpu.VMEM((ROWS, D), BF16),
            in_specs=[hbm] * len(args),
            out_specs=pl.BlockSpec(memory_space=pltpu.VMEM),
            scratch_shapes=[
                pltpu.VMEM((STAGES, STAGE_ROWS, 3, HEADS, HEAD_DIM), BF16),
                pltpu.VMEM((ROWS, D), BF16),
                pltpu.VMEM((4, ROWS, D), BF16),
                pltpu.VMEM((4, ROWS, D), BF16),
                pltpu.VMEM((4, ROWS, PK), BF16),
                pltpu.VMEM((4, ROWS, PK), BF16),
                pltpu.VMEM((4, ROWS, FF), F32),
                pltpu.VMEM((TOKENS, QKV), BF16),
                pltpu.VMEM((TOKENS, HEADS * HEAD_DIM), BF16),
                pltpu.VMEM((TOKENS, FF), BF16),
                pltpu.VMEM((3, ROWS, DIRECT), BF16),
                pltpu.VMEM((3, ROWS, DIRECT), BF16),
                *rs_buffers,
                *rs_buffers,
                pltpu.VMEM((4, 8, 128), F32),
                pltpu.VMEM((4, ROWS, 128), F32),
                pltpu.VMEM((128, 128), F32),
                pltpu.VMEM((4, 32, 128), F32),
                pltpu.VMEM((3, 32, 128), BF16),
                pltpu.VMEM((3, HEADS, HEAD_DIM), BF16),
                pltpu.VMEM((7, 1, D), F32),
                pltpu.VMEM((1, QKV), F32),
                pltpu.VMEM((TOKENS, TOKENS), F32),
                dma((STAGES,)), dma((RING,)), dma((5,)), dma((8,)), dma((3, len(AG2_CHUNKS))), dma((2,)), dma((2, NN + 1)),
                *[pltpu.VMEM((4, PK, PN), BF16)] * RING,
            ],
            compiler_params=pltpu.CompilerParams(collective_id=0, has_side_effects=True, vmem_limit_bytes=62 * 2**20),
            name="decoder_layer",
        )(*args)
        return result.reshape(hidden.shape)

    in_layout = (P("dp", "tp", None), P(), P(), P(None, None, "tp", None), P(None, "tp", None), P("tp", None, None), P(), P(), P(), P(None, "tp"), P("tp"), P("tp", None), P())
    return jax.shard_map(device_body, mesh=mesh, in_specs=in_layout, out_specs=P("dp", "tp", None), check_vma=False)
```

```python
import math

import jax
import jax.numpy as jnp
from jax import lax
from jax.experimental import pallas as pl
from jax.experimental.pallas import tpu as pltpu
from jax.sharding import PartitionSpec as P

MESH = pl.DeviceIdType.MESH
F32, BF16 = jnp.float32, jnp.bfloat16

LN_EPS = 1e-5
N_BATCH, BLOCK, D = 3, 16, 4096
ROWS = N_BATCH * BLOCK
TOKENS = 4 * ROWS
HEADS, HEAD_DIM = 8, 128
FF = 4096
QKV = 3 * HEADS * HEAD_DIM

PK, PN = 1024, 512
DIRECT = 256
NK, NN = D // PK, D // PN
AG1_CHUNKS = [(k * PK, PK) for k in range(NK)]
AG2_CHUNKS = [(0, 1024), (1024, 512), (1536, 1024), (2560, 1024), (3584, 512)]
RS1_CHUNKS = [(DIRECT, PN - DIRECT)] + [(n * PN, PN) for n in range(1, NN)]
RS2_CHUNKS = [(n * PN, PN) for n in range(NN)]
RING = 9
G_OUT, G_UP, G_DOWN, G_END = 6, 8, 16, 24
STAGE_ROWS, STAGES = 256, 4
STEPS = D // STAGE_ROWS


def kernel(x_hbm, g1_hbm, b1_hbm, wqkv_hbm, bqkv_hbm, wout_hbm, bout_hbm, g2_hbm, b2_hbm, wup_hbm, bup_hbm, wdown_hbm, bdown_hbm, out_ref,
           stage, x_own, h_all, x1_all, h2_even, h2_odd, acc, qkv_bf, ctx, u,
           dsend, drec, psend1, prec1, xsend1, xrec1, psend2, prec2, xsend2, xrec2, stats, stat_cols, square,
           vec_f32, vec_bf, bqkv_v, rows, bqkv_row, mask,
           ring_sem, send_sem, gather_sem, st_sem, rs_sem, *ring):
    dp = lax.axis_index("dp")
    me = lax.axis_index("tp")
    core = lax.rem(me, 2)
    chip = lax.div(me, 2)
    partner = me + 1 - 2 * core
    cross = lax.rem(me + 2, 4)
    far = lax.rem(partner + 2, 4)
    other_core = 1 - core
    other_chip = 1 - chip
    SEND_AG1, SEND_AG2, SEND_ST, SEND_RS1, SEND_RS2, SEND_DIRECT = 0, 1, 2, 3, 5, 7

    def remote(src, dst, send, recv, peer):
        return pltpu.make_async_remote_copy(src_ref=src, dst_ref=dst, send_sem=send, recv_sem=recv, device_id=(dp, peer), device_id_type=MESH)

    def stage_copy(i):
        return pltpu.make_async_copy(wqkv_hbm.at[pl.ds(i * STAGE_ROWS, STAGE_ROWS)], stage.at[lax.rem(i, STAGES)], rs_sem.at[0, 4 + lax.rem(i, STAGES)])

    def load_group(g):
        to, sem = ring[g % RING], ring_sem.at[g % RING]
        if g >= G_END:
            return
        if g >= G_DOWN:
            pltpu.make_async_copy(wdown_hbm.at[:, :, pl.ds((g - G_DOWN) * PN, PN)], to, sem).start()
            return
        for m in range(4):
            if g >= G_UP:
                k, n = (g - G_UP) // 2, (g - G_UP) % 2 * 4 + m
                src = wup_hbm.at[pl.ds(k * PK, PK), pl.ds(n * PN, PN)]
            else:
                src = wout_hbm.at[:, pl.ds(((g - G_OUT) * 4 + m) * PN, PN)]
            pltpu.make_async_copy(src, to.at[m], sem).start()

    def await_group(g):
        pltpu.make_async_copy(wdown_hbm.at[:, :, pl.ds(0, PN)], ring[g % RING], ring_sem.at[g % RING]).wait()

    barrier = pltpu.get_barrier_semaphore()
    for peer in (partner, cross, far):
        pl.semaphore_signal(barrier, inc=1, device_id=(dp, peer), device_id_type=MESH)
    G1, B1, G2, B2, BOUT, BUP, BDOWN = range(7)
    x_copy = pltpu.make_async_copy(x_hbm, x_own, st_sem.at[0])
    x_copy.start()
    for i, src in enumerate((g1_hbm, b1_hbm)):
        pltpu.make_async_copy(src, vec_f32.at[i], rs_sem.at[0, 0]).start()
    stage_copy(0).start()

    def f32_row(i):
        for j in range(32):
            rows[i, :, j * 128:(j + 1) * 128] = vec_f32[i, j:j + 1, :]

    def row_stats(x):
        mean = jnp.mean(x, axis=-1, keepdims=True)
        centered = x - mean
        var = jnp.mean(centered * centered, axis=-1, keepdims=True)
        return mean, lax.rsqrt(var + LN_EPS)

    pltpu.make_async_copy(vec_f32.at[pl.ds(2, 2)], vec_f32.at[pl.ds(0, 2)], rs_sem.at[0, 0]).wait()
    for i in (G1, B1):
        f32_row(i)
    stage_copy(1).start()
    x_copy.wait()
    for i in range(2, STAGES):
        stage_copy(i).start()
    for i, src in enumerate((g2_hbm, b2_hbm)):
        pltpu.make_async_copy(src, vec_f32.at[2 + i], rs_sem.at[0, 1]).start()
    for i, src in enumerate((bout_hbm, bup_hbm, bdown_hbm)):
        pltpu.make_async_copy(src, vec_bf.at[i], rs_sem.at[0, 2]).start()
    bqkv_copy = pltpu.make_async_copy(bqkv_hbm, bqkv_v, rs_sem.at[0, 3])
    bqkv_copy.start()
    for b in range(N_BATCH):
        r = pl.ds(b * BLOCK, BLOCK)
        xf = x_own[r, :].astype(F32)
        mean, rstd = row_stats(xf)
        h_all[me, r, :] = ((xf - mean) * rstd * rows[G1] + rows[B1]).astype(BF16)

    pl.semaphore_wait(barrier, 3)

    PARTNER, CROSS, FAR = range(3)

    def push(buf, chunks, send, which, block, peer, c):
        ref = buf.at[block, :, pl.ds(*chunks[c])]
        return remote(ref, ref, send_sem.at[send], gather_sem.at[which, c], peer)

    def ag1(which, block, peer, c):
        return push(h_all, AG1_CHUNKS, SEND_AG1, which, block, peer, c)

    def ag1_partner(block):
        return remote(h_all.at[block], h_all.at[block], send_sem.at[SEND_AG1], gather_sem.at[PARTNER, 0], partner)

    for c in range(NK):
        ag1(CROSS, me, cross, c).start()
    ag1_partner(me).start()

    def ag1_forward(c):
        ag1(CROSS, cross, cross, c).wait_recv()
        ag1(FAR, cross, partner, c).start()

    def relayout(k, off):
        s = lax.rem(k * 4 + off, STAGES)
        r = pl.ds(pl.multiple_of(off * STAGE_ROWS, STAGE_ROWS), STAGE_ROWS)
        for t in range(3):
            w = stage[s, :, t].reshape(STAGE_ROWS, HEADS * HEAD_DIM)
            for half in range(2):
                p = k * 6 + 2 * t + half
                ring[p // 4][p % 4, r, :] = w[:, half * PN:(half + 1) * PN]

    def relayout_chunk(k):
        def step(off, carry):
            stage_copy(k * 4 + off).wait()
            relayout(k, off)
            if k < NK - 1:
                stage_copy(k * 4 + off + STAGES).start()
            return carry

        lax.fori_loop(0, 4, step, 0)

    for k in range(3):
        relayout_chunk(k)
    pltpu.make_async_copy(vec_f32.at[pl.ds(0, 2)], vec_f32.at[pl.ds(2, 2)], rs_sem.at[0, 1]).wait()
    pltpu.make_async_copy(vec_bf, vec_bf, rs_sem.at[0, 2]).wait()
    bqkv_copy.wait()
    for i in (G2, B2):
        f32_row(i)
    for i in range(3):
        vals = vec_bf[i].astype(F32)
        for j in range(32):
            rows[4 + i, :, j * 128:(j + 1) * 128] = vals[j:j + 1, :]
    for t in range(3):
        vals = bqkv_v[t].astype(F32)
        for j in range(HEADS):
            bqkv_row[:, (t * HEADS + j) * 128:(t * HEADS + j + 1) * 128] = vals[j:j + 1, :]

    def token_place(axis):
        t = lax.broadcasted_iota(jnp.int32, (TOKENS, TOKENS), axis)
        d = sum((t >= ROWS * i).astype(jnp.int32) for i in range(1, 4))
        t = t - ROWS * d
        b = sum((t >= BLOCK * i).astype(jnp.int32) for i in range(1, N_BATCH))
        return b, d * BLOCK + t - BLOCK * b

    (q_seq, q_pos), (k_seq, k_pos) = token_place(0), token_place(1)
    square[...] = jnp.zeros_like(square)
    mask[...] = jnp.where(q_seq == k_seq, jnp.where(q_pos >= k_pos, 0.0, -1e30), -jnp.inf).astype(F32)
    ag1_forward(0)
    ag1_forward(1)
    relayout_chunk(3)
    for g in range(G_OUT, RING):
        load_group(g)
    def all_rows(ref, start, size):
        return ref[:, :, start:start + size].reshape(TOKENS, size)

    def part_of(t, j):
        return qkv_bf[:, (t * HEADS + j) * HEAD_DIM:(t * HEADS + j + 1) * HEAD_DIM]

    def scores(heads):
        return [lax.dot_general(part_of(0, j), part_of(1, j), (((1,), (1,)), ((), ())), preferred_element_type=F32) for j in heads]

    def softmax(logits):
        fill = mask[...]
        logits = [jnp.where(fill == 0.0, x * HEAD_DIM ** -0.5, fill) for x in logits]
        tops = [jnp.max(x, axis=-1, keepdims=True) for x in logits]
        es = [jnp.exp(x - t) for x, t in zip(logits, tops)]
        sums = [jnp.sum(e, axis=-1, keepdims=True) for e in es]
        return [(e * (1.0 / z)).astype(BF16) for e, z in zip(es, sums)]

    def weigh(heads, ps):
        for j, p in zip(heads, ps):
            ctx[:, j * HEAD_DIM:(j + 1) * HEAD_DIM] = jnp.dot(p, part_of(2, j), preferred_element_type=F32).astype(BF16)

    def qkv_block(chunks):
        for c in chunks:
            ag1(FAR, far, partner, c).wait_recv()
        first, last = chunks[0] == 0, chunks[-1] == NK - 1
        early = None
        for n in (0, 2, 4, 1, 3, 5):
            part = None if first else all_rows(acc, n * PN, PN)
            for c in chunks:
                p = c * 6 + n
                term = jnp.dot(all_rows(h_all, *AG1_CHUNKS[c]), ring[p // 4][p % 4], preferred_element_type=F32)
                part = term if part is None else part + term
            if last:
                qkv_bf[:, n * PN:(n + 1) * PN] = (part + bqkv_row[:, n * PN:(n + 1) * PN]).astype(BF16)
                if n == 4:
                    early = scores(range(4))
                if n in (1, 3):
                    half = softmax(early[:2])
                    early = early[2:]
                    weigh(range(n - 1, n + 1), half)
            else:
                acc[:, :, n * PN:(n + 1) * PN] = part.reshape(4, ROWS, PN)
        for g in range(chunks[0] * 6 // 4, (chunks[-1] + 1) * 6 // 4):
            load_group(g + RING)

    ag1_partner(partner).wait_recv()
    ag1_forward(2)
    qkv_block((0,))
    ag1_forward(3)
    qkv_block((1,))
    qkv_block((2, 3))

    ps = softmax(scores(range(4, 8)))
    weigh(range(4, 8), ps)

    def reduction(chunks, psend, prec, xsend, xrec, send):
        def pair(n):
            at = (slice(None), slice(None), pl.ds(*chunks[n]))
            return remote(psend.at[at], prec.at[at], send_sem.at[send], rs_sem.at[0, n], partner)

        def across(n):
            at = (slice(None), pl.ds(*chunks[n]))
            return remote(xsend.at[at], xrec.at[at], send_sem.at[send + 1], rs_sem.at[1, n], cross)

        def to_pair(n):
            cols = pl.ds(*chunks[n])
            for q in range(2):
                psend[q, :, cols] = acc[2 * q + other_core, :, cols].astype(BF16)
            pair(n).start()

        def to_cross(n):
            cols = pl.ds(*chunks[n])
            pair(n).wait_recv()
            xsend[:, cols] = (acc[2 * other_chip + core, :, cols] + prec[other_chip, :, cols].astype(F32)).astype(BF16)
            across(n).start()

        def total(n):
            cols = pl.ds(*chunks[n])
            across(n).wait_recv()
            return acc[me, :, cols] + prec[chip, :, cols].astype(F32) + xrec[:, cols].astype(F32)

        def drain():
            rest = pl.ds(chunks[0][0], D - chunks[0][0])
            at, sems = (slice(None), slice(None), rest), (send_sem.at[send], rs_sem.at[0, 0])
            remote(psend.at[at], prec.at[at], *sems, partner).wait_send()
            at, sems = (slice(None), rest), (send_sem.at[send + 1], rs_sem.at[1, 0])
            remote(xsend.at[at], xrec.at[at], *sems, cross).wait_send()

        return to_pair, to_cross, total, drain

    NR = len(RS1_CHUNKS)
    rs1_pair, rs1_cross, rs1_total, rs1_drain = reduction(RS1_CHUNKS, psend1, prec1, xsend1, xrec1, SEND_RS1)
    rs2_pair, rs2_cross, rs2_total, rs2_drain = reduction(RS2_CHUNKS, psend2, prec2, xsend2, xrec2, SEND_RS2)

    def ag2(which, block, peer, c):
        return push(x1_all, AG2_CHUNKS, SEND_AG2, which, block, peer, c)

    def st(block, peer, sem):
        return remote(stats.at[block], stats.at[block], send_sem.at[SEND_ST], st_sem.at[sem], peer)

    def direct(i):
        return remote(dsend.at[i], drec.at[i], send_sem.at[SEND_DIRECT], rs_sem.at[0, NR], (cross, far, partner)[i])

    def direct_total():
        remote(dsend, drec, send_sem.at[SEND_DIRECT], rs_sem.at[0, NR], cross).wait_recv()
        total = acc[me, :, 0:DIRECT]
        for i in (2, 0, 1):
            total = total + drec[i].astype(F32)
        return total

    ctx_rows = ctx[...]
    lead = 2
    for g in range(G_OUT, G_UP):
        await_group(g)
    for n in range(NR):
        part = jnp.dot(ctx_rows, ring[(G_OUT + n // 4) % RING][n % 4], preferred_element_type=F32)
        acc[:, :, n * PN:(n + 1) * PN] = part.reshape(4, ROWS, PN)
        if n == 0:
            for i, peer in enumerate((cross, far, partner)):
                dsend[i] = acc[peer, :, 0:DIRECT].astype(BF16)
            for i in range(3):
                direct(i).start()
        rs1_pair(n)
        if n >= lead:
            rs1_cross(n - lead)
    for g in range(G_OUT, G_UP):
        load_group(g + RING)
    for n in range(NR - lead, NR):
        rs1_cross(n)
    for n, (start, size) in enumerate([(0, DIRECT)] + RS1_CHUNKS):
        cols = pl.ds(start, size)
        total = rs1_total(n - 1) if n else direct_total()
        x1 = (x_own[:, cols].astype(F32) + (total + rows[BOUT, :, cols])).astype(BF16)
        x1_all[me, :, cols] = x1
        x1 = x1.astype(F32)
        part_mean = jnp.mean(x1, axis=-1, keepdims=True)
        part_dist = jnp.sum((x1 - part_mean) * (x1 - part_mean), axis=-1, keepdims=True)
        if n == 0:
            mean, dist = part_mean, part_dist
        else:
            step = part_mean - mean
            mean = mean + step * (size / (start + size))
            dist = dist + part_dist + step * step * (start * size / (start + size))
        if start + size == sum(AG2_CHUNKS[0]):
            ag2(CROSS, me, cross, 0).start()
            ag2(PARTNER, me, partner, 0).start()
    lane = lax.broadcasted_iota(jnp.int32, (ROWS, 128), 1)
    square[0:ROWS, :] = jnp.where(lane == 0, mean, lax.rsqrt(dist * (1.0 / D) + LN_EPS))
    stats[me] = square[...].T[:8]
    for peer in (cross, far):
        st(me, peer, 1).start()
    st(me, partner, 0).start()
    for c in range(1, len(AG2_CHUNKS)):
        ag2(CROSS, me, cross, c).start()
        ag2(PARTNER, me, partner, c).start()

    def ag2_forward(c):
        ag2(CROSS, cross, cross, c).wait_recv()
        ag2(FAR, cross, partner, c).start()

    def normalize(c, blocks):
        start, size = AG2_CHUNKS[c]
        cols = pl.ds(start, size)
        to = (h2_even, h2_odd)[c % 2]
        for d in blocks:
            xf = x1_all[d, :, cols].astype(F32)
            to[d, :, 0:size] = ((xf - stat_cols[d, :, 0:1]) * stat_cols[d, :, 1:2] * rows[G2, :, cols] + rows[B2, :, cols]).astype(BF16)

    def gelu(x):
        scale = (2 / math.pi) ** 0.5
        halved = 0.5 * x
        return halved + halved * jnp.tanh(x * (scale + (scale * 0.044715) * (x * x)))

    def blocks_of(c):
        start, size = AG2_CHUNKS[c]
        edges = sorted({start, start + size} | {k * PK for k in range(NK) if start < k * PK < start + size})
        return [(lo // PK, lo % PK, hi - lo) for lo, hi in zip(edges, edges[1:])]

    def up_panels(c, panels):
        h = all_rows((h2_even, h2_odd)[c % 2], 0, AG2_CHUNKS[c][1])
        for n in panels:
            part, done = all_rows(acc, n * PN, PN) if c else rows[BUP, :, n * PN:(n + 1) * PN], 0
            total = None
            for k, row, size in blocks_of(c):
                term = jnp.dot(h[:, done:done + size], ring[(G_UP + k * 2 + n // 4) % RING][n % 4, row:row + size, :], preferred_element_type=F32)
                total, done = term if total is None else total + term, done + size
            part = total + part
            if c < len(AG2_CHUNKS) - 1:
                acc[:, :, n * PN:(n + 1) * PN] = part.reshape(4, ROWS, PN)
            else:
                u[:, n * PN:(n + 1) * PN] = gelu(part).astype(BF16)

    def down_sum(n):
        total = None
        for k in range(NK):
            term = jnp.dot(u[:, k * PK:(k + 1) * PK], ring[(G_DOWN + n) % RING][k], preferred_element_type=F32)
            total = term if total is None else total + term
        return total

    def down_to_pair(n):
        acc[:, :, n * PN:(n + 1) * PN] = down_sum(n).reshape(4, ROWS, PN)
        rs2_pair(n)

    def columns(d):
        square[0:8, :] = stats[d]
        stat_cols[d] = square[...].T[:ROWS]

    st(partner, partner, 0).wait_recv()
    columns(me)
    columns(partner)
    ag2(PARTNER, partner, partner, 0).wait_recv()
    normalize(0, (me, partner))
    ag2_forward(0)
    remote(stats.at[pl.ds(0, 2)], stats.at[pl.ds(0, 2)], send_sem.at[SEND_ST], st_sem.at[1], cross).wait_recv()
    columns(cross)
    columns(far)
    ag2(FAR, far, partner, 0).wait_recv()
    normalize(0, (cross, far))
    for c in range(len(AG2_CHUNKS) - 1):
        for k, row, size in blocks_of(c):
            if row == 0:
                await_group(G_UP + 2 * k)
                await_group(G_UP + 2 * k + 1)
        before = (3, 5, 4, 0)[c]
        up_panels(c, range(before))
        ag2_forward(c + 1)
        ag2(PARTNER, partner, partner, c + 1).wait_recv()
        normalize(c + 1, (me, partner, cross))
        up_panels(c, range(before, NN))
        for k, row, size in blocks_of(c):
            if row + size == PK:
                load_group(G_UP + 2 * k + RING)
                load_group(G_UP + 2 * k + 1 + RING)
        ag2(FAR, far, partner, c + 1).wait_recv()
        normalize(c + 1, (far,))

    await_group(G_DOWN)
    up_panels(len(AG2_CHUNKS) - 1, range(NN))
    down_to_pair(0)
    load_group(G_DOWN - 2 + RING)
    load_group(G_DOWN - 1 + RING)
    for n in range(1, NR):
        await_group(G_DOWN + n)
        down_to_pair(n)
        rs2_cross(n - 1)
    rs2_cross(NR - 1)
    for n, (start, size) in enumerate(RS2_CHUNKS):
        cols = pl.ds(start, size)
        out_ref[:, cols] = (x1_all[me, :, cols].astype(F32) + (rs2_total(n) + rows[BDOWN, :, cols])).astype(BF16)

    for buf, send in ((h_all, SEND_AG1), (x1_all, SEND_AG2), (stats, SEND_ST)):
        remote(buf.at[pl.ds(0, 3)], buf.at[pl.ds(0, 3)], send_sem.at[send], st_sem.at[0], partner).wait_send()
    rs1_drain()
    remote(dsend, drec, send_sem.at[SEND_DIRECT], rs_sem.at[0, NR], cross).wait_send()
    rs2_drain()


def solution(mesh):
    def device_body(hidden, ln1_gain, ln1_bias, w_qkv, b_qkv, w_out, b_out, ln2_gain, ln2_bias, w_up, b_up, w_down, b_down):
        args = (hidden.reshape(ROWS, D), ln1_gain.reshape(32, 128), ln1_bias.reshape(32, 128), w_qkv, b_qkv, w_out.reshape(HEADS * HEAD_DIM, D),
                b_out.reshape(32, 128), ln2_gain.reshape(32, 128), ln2_bias.reshape(32, 128), w_up, b_up.reshape(32, 128), w_down.reshape(NK, PK, D), b_down.reshape(32, 128))
        hbm = pl.BlockSpec(memory_space=pltpu.HBM)
        dma = pltpu.SemaphoreType.DMA
        rs_buffers = [pltpu.VMEM((2, ROWS, D), BF16), pltpu.VMEM((2, ROWS, D), BF16), pltpu.VMEM((ROWS, D), BF16), pltpu.VMEM((ROWS, D), BF16)]
        result = pl.pallas_call(
            kernel,
            out_shape=pltpu.VMEM((ROWS, D), BF16),
            in_specs=[hbm] * len(args),
            out_specs=pl.BlockSpec(memory_space=pltpu.VMEM),
            scratch_shapes=[
                pltpu.VMEM((STAGES, STAGE_ROWS, 3, HEADS, HEAD_DIM), BF16),
                pltpu.VMEM((ROWS, D), BF16),
                pltpu.VMEM((4, ROWS, D), BF16),
                pltpu.VMEM((4, ROWS, D), BF16),
                pltpu.VMEM((4, ROWS, PK), BF16),
                pltpu.VMEM((4, ROWS, PK), BF16),
                pltpu.VMEM((4, ROWS, FF), F32),
                pltpu.VMEM((TOKENS, QKV), BF16),
                pltpu.VMEM((TOKENS, HEADS * HEAD_DIM), BF16),
                pltpu.VMEM((TOKENS, FF), BF16),
                pltpu.VMEM((3, ROWS, DIRECT), BF16),
                pltpu.VMEM((3, ROWS, DIRECT), BF16),
                *rs_buffers,
                *rs_buffers,
                pltpu.VMEM((4, 8, 128), F32),
                pltpu.VMEM((4, ROWS, 128), F32),
                pltpu.VMEM((128, 128), F32),
                pltpu.VMEM((4, 32, 128), F32),
                pltpu.VMEM((3, 32, 128), BF16),
                pltpu.VMEM((3, HEADS, HEAD_DIM), BF16),
                pltpu.VMEM((7, 1, D), F32),
                pltpu.VMEM((1, QKV), F32),
                pltpu.VMEM((TOKENS, TOKENS), F32),
                dma((RING,)), dma((8,)), dma((3, len(AG2_CHUNKS))), dma((2,)), dma((2, NN + 1)),
                *[pltpu.VMEM((4, PK, PN), BF16)] * RING,
            ],
            compiler_params=pltpu.CompilerParams(collective_id=0, has_side_effects=True, vmem_limit_bytes=62 * 2**20),
            name="decoder_layer",
        )(*args)
        return result.reshape(hidden.shape)

    in_layout = (P("dp", "tp", None), P(), P(), P(None, None, "tp", None), P(None, "tp", None), P("tp", None, None), P(), P(), P(), P(None, "tp"), P("tp"), P("tp", None), P())
    return jax.shard_map(device_body, mesh=mesh, in_specs=in_layout, out_specs=P("dp", "tp", None), check_vma=False)
```
